32 devices in a mesh: img: 4 (over y, core), proj: 8 (over z, x).
Axes of the slice: x: 2, y: 2, z: 4, core: 2. Of those that a mesh axis runs over, the one named last changes fastest.
Arguments:
- images: bfloat16 [512, 4096], P('img'), may hold values from -48 to 48
- projections: bfloat16 [2560, 4096], P('proj'), may hold values from -6 to 6
- noise_weight: float32 [4096], replicated, may hold values from 0.02 to 0.08
- defocus: float32 [512], P('img'), may hold values from 2 to 8
- orient_count: int32 [512], P('img'), may hold values from 160 to 2560, as said below
- term_limit: int32 [512], P('img'), may hold values from 2048 to 4096
- block_plan: int32 [16], replicated, may hold values from 0 to 15, each once
Outputs:
- reconstruction: bfloat16 [2560, 4096], P('proj', 'img')
- evidence_next: float32 [512], P('img')
The draws below stay inside these ranges and needn't reach their ends.
Inputs may be any that keep to these rules, and one draw needn't show every extreme that they name: Orientations 0 to orient_count[i] - 1 are the significant ones of image i; some image has all 2560.
All inputs are finite; a program needn't handle non-finite values.
Results may differ from the reference program's by a relative error of at most 0.018.
Values may be sent and summed in bfloat16 or wider, within the bound.
A program may use at most 64 MiB of HBM per device.

```python
import math
import jax
import jax.numpy as jnp
from jax import lax

F = 4096
NPROJ = 2560
IMG_DEV = 128
BLOCK = 32
NIMG = 512
NBLK = 16
N_IMG = 4


def shared_draw(key):
    projections = jnp.clip(jax.random.normal(jax.random.fold_in(key, 101), (NPROJ, F), jnp.float32), -6.0, 6.0)
    defocus = jax.random.uniform(jax.random.fold_in(key, 102), (NIMG,), jnp.float32, 2.0, 8.0)
    pixels = jnp.clip(jax.random.normal(jax.random.fold_in(key, 103), (NIMG, F), jnp.float32), -6.0, 6.0)
    return (projections, defocus, pixels)


def draw_projections(key, part):
    return shared_draw(key)[0].astype(jnp.bfloat16)


def draw_defocus(key, part):
    return shared_draw(key)[1]


def draw_images(key, part):
    projections, defocus, pixels = shared_draw(key)
    row_ids = jnp.arange(NIMG, dtype=jnp.int32)
    chosen = row_ids % 16 == 5
    first_pick = jax.random.randint(jax.random.fold_in(key, 105), (NIMG,), 0, max(NPROJ // 16 - 1, 1))
    second_pick = first_pick + 1
    strength = jnp.array([2.0, 3.0, 4.0], jnp.float32)[row_ids // 16 % 3]
    frequency = (jnp.arange(F, dtype=jnp.float32) + 1.0) / F
    contrast = jnp.sin(2.0 * math.pi * defocus[:, None] * frequency[None, :] + 0.1)
    aligned = strength[:, None] * contrast * (projections[first_pick] + projections[second_pick])
    pixels = jnp.where(chosen[:, None], aligned, pixels)
    return pixels.astype(jnp.bfloat16)


def draw_orient_count(key, part):
    lowest = NPROJ // 16
    level = jax.random.randint(jax.random.fold_in(key, 201), (NIMG // IMG_DEV,), lowest, NPROJ + 1)
    level = jnp.repeat(level, IMG_DEV)
    spread = jax.random.randint(jax.random.fold_in(key, 202), (NIMG,), 0, 1 << 20)
    counts = lowest + spread % (level - lowest + 1)
    return counts.at[0].set(NPROJ).astype(jnp.int32)


def place_ends(values, stream_key, smallest, high):
    shape = values.shape
    place = [jax.random.randint(jax.random.fold_in(stream_key, axis), (), 0, shape[axis]) for axis in range(len(shape))]
    values = values.at[tuple(place)].set(smallest)
    longest = shape.index(max(shape))
    place[longest] = (place[longest] + 1) % shape[longest]
    return values.at[tuple(place)].set(high)


def setup_inputs(seed: int = 0) -> dict:
    streams_of = jax.random.split(jax.random.key(seed), 8)
    return {
        "images": draw_images(jax.random.fold_in(streams_of[7], 71), 0),
        "projections": draw_projections(jax.random.fold_in(streams_of[7], 71), 0),
        "noise_weight": jnp.clip(jnp.exp(jax.random.uniform(streams_of[2], (F,), jnp.float32, math.log(0.02), math.log(0.08))), 0.02, 0.08),
        "defocus": draw_defocus(jax.random.fold_in(streams_of[7], 71), 0),
        "orient_count": draw_orient_count(jax.random.fold_in(streams_of[7], 71), 0),
        "term_limit": place_ends(jax.random.randint(streams_of[5], (NIMG,), F // 2, F + 1), jax.random.fold_in(streams_of[5], 1), F // 2, F).astype(jnp.int32),
        "block_plan": jax.random.permutation(streams_of[6], NBLK).astype(jnp.int32),
    }


def contrast_table(defocus, width):
    frequency = (jnp.arange(width, dtype=jnp.float32) + 1.0) / width
    return jnp.sin(2.0 * math.pi * defocus[:, None] * frequency[None, :] + 0.1)


def image_terms(pixels, noise_weight, defocus, limits):
    width = pixels.shape[1]
    contrast = contrast_table(defocus, width)
    keep_mask = (jnp.arange(width, dtype=jnp.int32)[None, :] < limits[:, None]).astype(contrast.dtype)
    values = pixels.astype(contrast.dtype)
    weighted = (keep_mask * noise_weight[None, :] * contrast * values).astype(jnp.bfloat16)
    weighted_sq = (keep_mask * noise_weight[None, :] * contrast * contrast).astype(jnp.bfloat16)
    back_images = (keep_mask * contrast * values).astype(jnp.bfloat16)
    back_weights = (keep_mask * contrast * contrast).astype(jnp.bfloat16)
    return weighted, weighted_sq, back_images, back_weights


def reference(images, projections, noise_weight, defocus, orient_count, term_limit, block_plan):
    wide = projections.astype(jnp.float32)
    proj_sq = (wide * wide).astype(jnp.bfloat16)
    orient_ids = jnp.arange(NPROJ, dtype=jnp.int32)

    def one_block(totals, segment):
        pixels, focus, counts, limits = segment
        weighted, weighted_sq, back_images, back_weights = image_terms(pixels, noise_weight, focus, limits)
        scores = jnp.dot(projections, weighted.T, preferred_element_type=jnp.float32)
        scores = scores - 0.5 * jnp.dot(proj_sq, weighted_sq.T, preferred_element_type=jnp.float32)
        significant = orient_ids[:, None] < counts[None, :]
        row_peak = jnp.max(jnp.where(significant, scores, -1e30), axis=0)
        safe = jnp.where(significant, scores, row_peak[None, :])
        row_mass = jnp.sum(jnp.where(significant, jnp.exp(safe - row_peak[None, :]), 0.0), axis=0)
        log_evidence = row_peak + jnp.log(row_mass)
        posterior = jnp.where(significant, jnp.exp(safe - log_evidence[None, :]), 0.0).astype(jnp.bfloat16)
        part_images = jnp.dot(posterior, back_images, preferred_element_type=jnp.float32).astype(jnp.bfloat16)
        part_weights = jnp.dot(posterior, back_weights, preferred_element_type=jnp.float32).astype(jnp.bfloat16)
        part_images = lax.optimization_barrier(part_images).astype(totals[0].dtype)
        part_weights = lax.optimization_barrier(part_weights).astype(totals[1].dtype)
        return (totals[0] + part_images, totals[1] + part_weights), log_evidence

    segments = (images.reshape(N_IMG, IMG_DEV, F), defocus.reshape(N_IMG, IMG_DEV),
                orient_count.reshape(N_IMG, IMG_DEV), term_limit.reshape(N_IMG, IMG_DEV))
    empty_sum = jnp.zeros((NPROJ, F), jnp.float32)
    (sum_images, sum_weights), evidence = lax.scan(one_block, (empty_sum, empty_sum), segments)
    reconstruction = (sum_images / (sum_weights + 1.0)).astype(jnp.bfloat16)
    evidence = evidence.reshape(NBLK, BLOCK)
    placed = jnp.zeros_like(evidence).at[block_plan].set(evidence)
    return reconstruction, placed.reshape(NIMG)
```

```python
import functools
import math

import jax
import jax.numpy as jnp
from jax import lax
from jax.experimental import pallas as pl
from jax.experimental.pallas import tpu as pltpu
from jax.sharding import PartitionSpec as P

BLOCK = 32
PIECES = 2
LANES = 128
DEPTH = 512
LOADS = 4
MESH = pl.DeviceIdType.MESH
SIN_TERMS = [(-1.0) ** k * math.pi ** (2 * k + 1) / math.factorial(2 * k + 1) for k in range(7)]
COS_TERMS = [(-1.0) ** k * math.pi ** (2 * k) / math.factorial(2 * k) for k in range(8)]


def horner(terms, x):
    total = jnp.full_like(x, terms[-1])
    for term in terms[-2::-1]:
        total = total * x + term
    return total


def sincos_turns(turns):
    rest = turns - jnp.floor(turns + 0.5)
    square = rest * rest
    half_sin = rest * horner(SIN_TERMS, square)
    half_cos = horner(COS_TERMS, square)
    return 2.0 * half_sin * half_cos, 1.0 - 2.0 * half_sin * half_sin


def columns_of(row, rows):
    return jnp.broadcast_to(row, (LANES, rows)).T


def sine_start(focus, term0, width):
    sin0, cos0 = sincos_turns(focus * ((term0 + 1.0) / width) + 0.1 / (2.0 * math.pi))
    sin_d, cos_d = sincos_turns(focus * (LANES / width))
    return sin0, sin0 * cos_d - cos0 * sin_d, 2.0 * cos_d


def wait_bytes(ref, sem):
    pltpu.make_async_copy(ref, ref, sem).wait()


def score_kernel(n_img, n_proj, x_size, img_hbm, proj_hbm, noise_hbm, focus_hbm, count_hbm, limit_hbm, plan_hbm,
                 posts_ref, back_img, back_wgt, ev_ref,
                 img, proj, noise_ref, focus_ref, count_ref, limit_ref, plan_ref, weighted, weighted_sq, total,
                 moved, contrast, focus_all, limit_all, terms, every_terms, stats, every_stats,
                 load_sem, img_load, proj_load, x_token, up_token, down_token,
                 small_send, small_recv, img_send, img_recv, pass_send, pass_recv,
                 post_send, post_recv, stat_send, stat_recv):
    me = lax.axis_index("img")
    mine = lax.axis_index("proj")
    img_rows, width = img.shape
    proj_rows = proj.shape[0]
    part = width // n_img
    chips = n_img // 2
    z_size = n_proj // x_size
    row_y, core = me // 2, lax.rem(me, 2)
    at_x, at_z = lax.rem(mine, x_size), mine // x_size

    def img_to(t):
        return lax.rem(row_y + t // 2, chips) * 2 + lax.rem(core + t % 2, 2)

    def img_from(t):
        return lax.rem(row_y + chips - t // 2, chips) * 2 + lax.rem(core + t % 2, 2)

    side = lax.rem(mine, 2)
    beside = mine + 1 - 2 * side
    piece = img_rows // 2 // PIECES
    x_peers = [at_z * x_size + lax.rem(at_x + k, x_size) for k in range(1, x_size)]
    bottom, top = at_z == 0, at_z == z_size - 1

    barrier = pltpu.get_barrier_semaphore()
    for t in range(1, n_img):
        pl.semaphore_signal(barrier, inc=1, device_id={"img": img_to(t)}, device_id_type=MESH)
    for peer in x_peers:
        pl.semaphore_signal(barrier, inc=1, device_id={"proj": peer}, device_id_type=MESH)

    def signal_up(sem):
        pl.semaphore_signal(sem, inc=1, device_id={"proj": mine + x_size}, device_id_type=MESH)

    def signal_down(sem):
        pl.semaphore_signal(sem, inc=1, device_id={"proj": mine - x_size}, device_id_type=MESH)

    pl.when(jnp.logical_not(top))(lambda: signal_up(barrier))
    pl.when(jnp.logical_not(bottom))(lambda: signal_down(barrier))

    small_loads = [pltpu.make_async_copy(source, target, load_sem.at[n]) for n, (source, target) in enumerate(
        ((focus_hbm, focus_ref), (limit_hbm, limit_ref), (noise_hbm, noise_ref), (count_hbm, count_ref),
         (plan_hbm, plan_ref)))]
    wide = width // LOADS
    img_loads = [pltpu.make_async_copy(img_hbm.at[:, pl.ds(n * wide, wide)], img.at[:, pl.ds(n * wide, wide)],
                                       img_load.at[n]) for n in range(LOADS)]
    proj_loads = [pltpu.make_async_copy(proj_hbm.at[:, pl.ds(n * wide, wide)], proj.at[:, pl.ds(n * wide, wide)],
                                        proj_load.at[n]) for n in range(LOADS)]
    for load in small_loads[:3]:
        load.start()
    for n in range(LOADS):
        img_loads[n].start()
        proj_loads[n].start()
    for load in small_loads[3:]:
        load.start()
    small_loads[0].wait()
    small_loads[1].wait()

    lane = lax.broadcasted_iota(jnp.int32, (1, LANES), 1).astype(jnp.float32)
    focus = columns_of(focus_ref[...], img_rows)
    limit = columns_of(limit_ref[...].astype(jnp.float32), img_rows)
    sin_v, sin_before, turn = sine_start(focus, lane, width)
    small_loads[2].wait()
    contract = (((1,), (1,)), ((), ()))
    small, moves = [], []

    def terms_chunk(c, sin_v, sin_before):
        for k in range(DEPTH // LANES):
            first = c * DEPTH + k * LANES
            cols = slice(first, first + LANES)
            kept = jnp.where(lane + float(first) < limit, sin_v, 0.0)
            noisy = kept * noise_ref[:, cols]
            weighted[:, cols] = (noisy * img[:, cols].astype(jnp.float32)).astype(jnp.bfloat16)
            weighted_sq[:, cols] = (noisy * (-0.5 * sin_v)).astype(jnp.bfloat16)
            sin_v, sin_before = turn * sin_v - sin_before, sin_v
        return sin_v, sin_before

    def score_chunk(c):
        cols = slice(c * DEPTH, (c + 1) * DEPTH)
        rows = proj[:, cols]
        got = lax.dot_general(rows, weighted[:, cols], contract, preferred_element_type=jnp.float32)
        got = got + lax.dot_general(rows * rows, weighted_sq[:, cols], contract, preferred_element_type=jnp.float32)
        if c:
            total[...] += got
        else:
            total[...] = got

    def start_img(n):
        for t in range(2, n_img):
            rows = pl.ds(pl.multiple_of((side * PIECES + n) * piece, piece), piece)
            slab = pl.ds(pl.multiple_of(img_to(t) * part, LANES), part)
            copy = pltpu.make_async_remote_copy(
                src_ref=img.at[rows, slab], dst_ref=moved.at[t, rows, :], send_sem=img_send.at[t, n],
                recv_sem=img_recv.at[t, n], device_id={"img": img_to(t)}, device_id_type=MESH)
            copy.start()
            moves.append((t, n, copy))

    chunks = width // DEPTH
    per_load = wide // DEPTH
    loaded = []

    def need_img(n):
        for k in range(len(loaded), n + 1):
            img_loads[k].wait()
            loaded.append(k)

    need_img(0)
    sin_v, sin_before = terms_chunk(0, sin_v, sin_before)
    near = None
    for c in range(chunks):
        if c + 1 < chunks:
            need_img((c + 1) // per_load)
            sin_v, sin_before = terms_chunk(c + 1, sin_v, sin_before)
        if c % per_load == 0:
            proj_loads[c // per_load].wait()
        score_chunk(c)
        if c == (chunks // 4 if chunks >= 8 else 0):
            pl.semaphore_wait(barrier, n_img + x_size - 2 + jnp.where(bottom, 0, 1) + jnp.where(top, 0, 1))
            for peer in x_peers:
                pl.semaphore_signal(x_token, inc=1, device_id={"proj": peer}, device_id_type=MESH)
            for t in range(1, n_img):
                for n, (ref, dst) in enumerate(((focus_ref, focus_all), (limit_ref, limit_all))):
                    small.append(pltpu.make_async_remote_copy(
                        src_ref=ref, dst_ref=dst.at[t], send_sem=small_send.at[n, t], recv_sem=small_recv.at[n, t],
                        device_id={"img": img_to(t)}, device_id_type=MESH))
                    small[-1].start()
        if c == chunks // 2:
            need_img(LOADS - 1)
            start_img(0)
            near = pltpu.make_async_remote_copy(
                src_ref=img.at[:, pl.ds(pl.multiple_of(img_to(1) * part, LANES), part)], dst_ref=moved.at[1],
                send_sem=img_send.at[1, 0], recv_sem=img_recv.at[1, 0], device_id={"img": img_to(1)},
                device_id_type=MESH)
            near.start()
            pl.semaphore_wait(x_token, x_size - 1)
            pl.when(bottom)(lambda: signal_up(up_token))
            pl.when(top)(lambda: signal_down(down_token))
            for n in range(1, PIECES):
                start_img(n)
        if c == chunks * 3 // 4:
            @pl.when(jnp.logical_not(bottom))
            def _():
                pl.semaphore_wait(up_token, 1)
                pl.when(jnp.logical_not(top))(lambda: signal_up(up_token))

    small_loads[3].wait()
    small_loads[4].wait()
    scores = total[...]
    orient = lax.broadcasted_iota(jnp.int32, (proj_rows, img_rows), 0) + mine * proj_rows
    significant = orient < count_ref[...]
    masked = jnp.where(significant, scores, -1e30)
    peak = jnp.max(masked, axis=0, keepdims=True)
    expo = jnp.where(significant, jnp.exp(masked - peak), 0.0)
    stats[0:1, :] = peak
    stats[1:2, :] = jnp.sum(expo, axis=0, keepdims=True)
    terms[...] = expo.astype(jnp.bfloat16)

    @pl.when(jnp.logical_not(top))
    def _():
        pl.semaphore_wait(down_token, 1)
        pl.when(jnp.logical_not(bottom))(lambda: signal_down(down_token))

    def send_stats(n, carry):
        t, j = n // n_proj, lax.rem(n, n_proj)
        pltpu.make_async_remote_copy(
            src_ref=stats, dst_ref=every_stats.at[n], send_sem=stat_send, recv_sem=stat_recv,
            device_id={"img": lax.rem(row_y + t // 2, chips) * 2 + lax.rem(core + lax.rem(t, 2), 2),
                       "proj": lax.rem(mine + j, n_proj)}, device_id_type=MESH).start()
        return carry

    lax.fori_loop(1, n_img * n_proj, send_stats, 0)
    post_copies = [pltpu.make_async_remote_copy(
        src_ref=terms, dst_ref=every_terms.at[t], send_sem=post_send.at[t], recv_sem=post_recv.at[t],
        device_id={"img": img_to(t)}, device_id_type=MESH) for t in range(1, n_img)]
    for copy in post_copies[::-1]:
        copy.start()

    term0 = lane + (me * part).astype(jnp.float32)

    def weights_block(t, focus_row, limit_row):
        limit_b = columns_of(limit_row.astype(jnp.float32), img_rows)
        sin_v, sin_before, turn = sine_start(columns_of(focus_row, img_rows), term0, width)
        rows = pl.ds(pl.multiple_of(t * img_rows, img_rows), img_rows)
        for c in range(part // LANES):
            cols = slice(c * LANES, (c + 1) * LANES)
            kept = jnp.where(term0 + float(c * LANES) < limit_b, sin_v, 0.0)
            contrast[rows, cols] = kept
            back_wgt[rows, cols] = (kept * sin_v).astype(jnp.bfloat16)
            sin_v, sin_before = turn * sin_v - sin_before, sin_v

    def take_images(t, pixels):
        rows = pl.ds(t * img_rows, img_rows)
        back_img[rows, :] = (contrast[rows, :] * pixels.astype(jnp.float32)).astype(jnp.bfloat16)

    focus_all[0] = focus_ref[...]
    limit_all[0] = limit_ref[...]
    for copy in small:
        copy.wait()

    def any_block(t, carry):
        weights_block(t, focus_all[t], limit_all[t])
        return carry

    lax.fori_loop(0, n_img, any_block, 0)
    passed = []

    def pass_on(t, n, copy):
        copy.wait()
        held = moved.at[t, pl.ds(pl.multiple_of((side * PIECES + n) * piece, piece), piece), :]
        passed.append(pltpu.make_async_remote_copy(
            src_ref=held, dst_ref=held, send_sem=pass_send.at[t, n], recv_sem=pass_recv.at[t, n],
            device_id={"proj": beside}, device_id_type=MESH))
        passed[-1].start()

    for move in moves[:n_img - 2]:
        pass_on(*move)
    take_images(0, img[:, pl.ds(pl.multiple_of(me * part, LANES), part)])
    near.wait()
    take_images(1, moved[1])
    for move in moves[n_img - 2:]:
        pass_on(*move)
    for copy in passed:
        copy.wait()
    for t in range(2, n_img):
        take_images(t, moved[t])

    every_stats[0] = stats[...]
    wait_bytes(every_stats.at[pl.ds(1, n_img * n_proj - 1)], stat_recv)
    wait_bytes(every_stats.at[pl.ds(1, n_img * n_proj - 1)], stat_send)
    evidence = []
    for t in range(n_img):
        every = every_stats[pl.ds(t * n_proj, n_proj)]
        peaks, masses = every[:, 0, :], every[:, 1, :]
        highest = jnp.max(peaks, axis=0, keepdims=True)
        whole = jnp.sum(masses * jnp.exp(peaks - highest), axis=0, keepdims=True)
        evidence.append(highest + jnp.log(whole))
        scale = jnp.exp(peaks[0:1, :] - evidence[t])
        if t:
            post_copies[t - 1].wait()
        values = every_terms[t].astype(jnp.float32) if t else expo
        posts_ref[:, t * img_rows:(t + 1) * img_rows] = (values * scale).astype(jnp.bfloat16)

    groups = img_rows // BLOCK
    group = lax.broadcasted_iota(jnp.int32, (1, img_rows), 1) // BLOCK
    placed = jnp.zeros((1, img_rows), jnp.float32)
    for t in range(n_img):
        plan = jnp.zeros((1, img_rows), jnp.int32)
        for g in range(groups):
            plan = jnp.where(group == g, plan_ref[img_from(t) * groups + g], plan)
        for s in range(groups):
            turned, target = evidence[t], plan
            if s:
                turned = pltpu.roll(evidence[t], s * BLOCK, 1)
                target = pltpu.roll(plan, s * BLOCK, 1)
            placed = placed + jnp.where(target == me * groups + group, turned, 0.0)
    ev_ref[...] = placed


def back_kernel(posts_ref, back_img, back_wgt, ev_ref, rec_hbm, placed_hbm, rec, out_sem):
    part = back_img.shape[1]
    step = min(part, 256)
    steps = part // step
    posts = posts_ref[...]
    last = pltpu.make_async_copy(ev_ref, placed_hbm, out_sem.at[steps])
    last.start()
    copies = [last]
    for c in range(steps):
        cols = slice(c * step, (c + 1) * step)
        sums = jnp.dot(posts, back_img[:, cols], preferred_element_type=jnp.float32)
        weights = jnp.dot(posts, back_wgt[:, cols], preferred_element_type=jnp.float32)
        rec[:, cols] = (sums / (weights + 1.0)).astype(jnp.bfloat16)
        copies.append(pltpu.make_async_copy(rec.at[:, cols], rec_hbm.at[:, cols], out_sem.at[c]))
        copies[-1].start()
    for copy in copies:
        copy.wait()


def shards(n_img, n_proj, images, projections, noise_weight, defocus, orient_count, term_limit, block_plan):
    img_rows, width = images.shape
    proj_rows = projections.shape[0]
    part = width // n_img
    x_size = 1 << ((n_proj.bit_length() - 1) // 2)
    vmem = pl.BlockSpec(memory_space=pltpu.VMEM)
    hbm = pl.BlockSpec(memory_space=pl.ANY)
    bf16, f32, i32 = jnp.bfloat16, jnp.float32, jnp.int32
    dma, regular = pltpu.SemaphoreType.DMA, pltpu.SemaphoreType.REGULAR
    held = pl.pallas_call(
        functools.partial(score_kernel, n_img, n_proj, x_size),
        out_shape=(pltpu.VMEM((proj_rows, n_img * img_rows), bf16), pltpu.VMEM((n_img * img_rows, part), bf16),
                   pltpu.VMEM((n_img * img_rows, part), bf16), pltpu.VMEM((1, img_rows), f32)),
        in_specs=[hbm] * 7,
        out_specs=(vmem, vmem, vmem, vmem),
        scratch_shapes=[
            pltpu.VMEM((img_rows, width), bf16),
            pltpu.VMEM((proj_rows, width), bf16),
            pltpu.VMEM((1, width), f32),
            pltpu.VMEM((1, img_rows), f32),
            pltpu.VMEM((1, img_rows), i32),
            pltpu.VMEM((1, img_rows), i32),
            pltpu.SMEM(block_plan.shape, i32),
            pltpu.VMEM((img_rows, width), bf16),
            pltpu.VMEM((img_rows, width), bf16),
            pltpu.VMEM((proj_rows, img_rows), f32),
            pltpu.VMEM((n_img, img_rows, part), bf16),
            pltpu.VMEM((n_img * img_rows, part), f32),
            pltpu.VMEM((n_img, 1, img_rows), f32),
            pltpu.VMEM((n_img, 1, img_rows), i32),
            pltpu.VMEM((proj_rows, img_rows), bf16),
            pltpu.VMEM((n_img, proj_rows, img_rows), bf16),
            pltpu.VMEM((2, img_rows), f32),
            pltpu.VMEM((n_img * n_proj, 2, img_rows), f32),
            dma((5,)), dma((LOADS,)), dma((LOADS,)), regular, regular, regular,
            dma((2, n_img)), dma((2, n_img)),
            dma((n_img, PIECES)), dma((n_img, PIECES)),
            dma((n_img, PIECES)), dma((n_img, PIECES)),
            dma((n_img,)), dma((n_img,)), dma, dma,
        ],
        compiler_params=pltpu.CompilerParams(
            collective_id=0, has_side_effects=True, vmem_limit_bytes=54 * 1024 * 1024),
    )(images, projections, noise_weight.reshape(1, -1), defocus.reshape(1, -1), orient_count.reshape(1, -1),
      term_limit.reshape(1, -1), block_plan)
    reconstruction, evidence = pl.pallas_call(
        back_kernel,
        out_shape=(jax.ShapeDtypeStruct((proj_rows, part), bf16), jax.ShapeDtypeStruct((1, img_rows), f32)),
        in_specs=[vmem] * 4,
        out_specs=(hbm, hbm),
        scratch_shapes=[pltpu.VMEM((proj_rows, part), bf16), dma((part // min(part, 256) + 1,))],
        compiler_params=pltpu.CompilerParams(vmem_limit_bytes=16 * 1024 * 1024),
    )(*held)
    return reconstruction, evidence.reshape(-1)


def solution(mesh):
    n_img, n_proj = mesh.shape["img"], mesh.shape["proj"]
    placed = (P("img", None), P("proj", None), P(), P("img"), P("img"), P("img"), P())
    return jax.shard_map(
        functools.partial(shards, n_img, n_proj), mesh=mesh, in_specs=placed,
        out_specs=(P("proj", "img"), P("img")), check_vma=False,
    )
```

```python
import functools
import math

import jax
import jax.numpy as jnp
from jax import lax
from jax.experimental import pallas as pl
from jax.experimental.pallas import tpu as pltpu
from jax.sharding import PartitionSpec as P

BLOCK = 32
PIECES = 4
LANES = 128
DEPTH = 512
NEAR_STEP = 1
MESH = pl.DeviceIdType.MESH
SIN_TERMS = [(-1.0) ** k * math.pi ** (2 * k + 1) / math.factorial(2 * k + 1) for k in range(7)]
COS_TERMS = [(-1.0) ** k * math.pi ** (2 * k) / math.factorial(2 * k) for k in range(8)]


def horner(terms, x):
    total = jnp.full_like(x, terms[-1])
    for term in terms[-2::-1]:
        total = total * x + term
    return total


def sincos_turns(turns):
    rest = turns - jnp.floor(turns + 0.5)
    square = rest * rest
    half_sin = rest * horner(SIN_TERMS, square)
    half_cos = horner(COS_TERMS, square)
    return 2.0 * half_sin * half_cos, 1.0 - 2.0 * half_sin * half_sin


def columns_of(row, rows):
    return jnp.broadcast_to(row, (LANES, rows)).T


def step_sines(row, width):
    sin_d, cos_d = sincos_turns(row * (LANES / width))
    rows = row.shape[1]
    return columns_of(sin_d, rows), columns_of(cos_d, rows)


def sine_start(row, term0, width):
    sin_d, cos_d = step_sines(row, width)
    focus = columns_of(row, row.shape[1])
    sin0, cos0 = sincos_turns(focus * ((term0 + 1.0) / width) + 0.1 / (2.0 * math.pi))
    return sin0, sin0 * cos_d - cos0 * sin_d, 2.0 * cos_d


def wait_bytes(ref, sem):
    pltpu.make_async_copy(ref, ref, sem).wait()


def score_kernel(n_img, n_proj, x_size, img_hbm, proj_hbm, noise_hbm, focus_hbm, count_hbm, limit_hbm, plan_hbm,
                 posts_ref, back_img, back_wgt, ev_ref,
                 img, proj, noise_ref, focus_ref, count_ref, limit_ref, plan_ref, weighted, weighted_sq, total,
                 sine, moved, contrast, focus_all, limit_all, terms, every_terms, stats, every_stats,
                 load_sem, img_load, proj_load, up_token, down_token,
                 small_send, small_recv, near_sem, img_send, img_recv, pass_send, pass_recv,
                 post_send, post_recv, stat_send, stat_recv):
    me = lax.axis_index("img")
    mine = lax.axis_index("proj")
    img_rows, width = img.shape
    proj_rows = proj.shape[0]
    part = width // n_img
    chips = n_img // 2
    z_size = n_proj // x_size
    row_y, core = me // 2, lax.rem(me, 2)
    at_x, at_z = lax.rem(mine, x_size), mine // x_size
    bottom, top = at_z == 0, at_z == z_size - 1

    def img_to(t):
        return lax.rem(row_y + t // 2, chips) * 2 + lax.rem(core + lax.rem(t, 2), 2)

    def img_from(t):
        return lax.rem(row_y + chips - t // 2, chips) * 2 + lax.rem(core + t % 2, 2)

    side = lax.rem(at_x + at_z, 2)
    across = (mine + 1 - 2 * lax.rem(at_x, 2), mine + x_size * (1 - 2 * lax.rem(at_z, 2)))
    piece = img_rows // 2 // PIECES

    def signal(sem, img, proj):
        pl.semaphore_signal(sem, inc=1, device_id={"img": img, "proj": proj}, device_id_type=MESH)

    barrier = pltpu.get_barrier_semaphore()
    for k in range(x_size):
        for t in range(n_img):
            if k or t:
                signal(barrier, img_to(t), at_z * x_size + lax.rem(at_x + k, x_size))
    pl.when(jnp.logical_not(top))(lambda: signal(barrier, me, mine + x_size))
    pl.when(jnp.logical_not(bottom))(lambda: signal(barrier, me, mine - x_size))

    small_loads = [pltpu.make_async_copy(source, target, load_sem.at[n]) for n, (source, target) in enumerate(
        ((focus_hbm, focus_ref), (limit_hbm, limit_ref), (noise_hbm, noise_ref), (count_hbm, count_ref),
         (plan_hbm, plan_ref)))]
    wide = 2 * DEPTH
    steps = width // wide

    def load_img(n):
        cols = pl.ds(pl.multiple_of(n * wide, wide), wide)
        return pltpu.make_async_copy(img_hbm.at[:, cols], img.at[:, cols], img_load.at[n])

    def load_proj(n):
        cols = pl.ds(pl.multiple_of(n * wide, wide), wide)
        return pltpu.make_async_copy(proj_hbm.at[:, cols], proj.at[:, cols], proj_load.at[n])

    for load in small_loads[:3]:
        load.start()
    load_img(0).start()
    for n in range(steps):
        load_proj(n).start()
        if n + 1 < steps:
            load_img(n + 1).start()
    for load in small_loads[3:]:
        load.start()
    with jax.named_scope("small"):
        small_loads[0].wait()
        small_loads[1].wait()

    lane = lax.broadcasted_iota(jnp.int32, (1, LANES), 1).astype(jnp.float32)
    sine[0], sine[1], sine[2] = sine_start(focus_ref[...], lane, width)
    sine[3] = columns_of(limit_ref[...].astype(jnp.float32), img_rows)
    total[...] = jnp.zeros_like(total)
    small_loads[2].wait()
    contract = (((1,), (1,)), ((), ()))
    strip = 16

    def terms_chunk(c, slot):
        starts = [pl.multiple_of(c * DEPTH + k * LANES, LANES) for k in range(DEPTH // LANES)]
        noise = [noise_ref[:, pl.ds(start, LANES)] for start in starts]
        term = [lane + start.astype(jnp.float32) for start in starts]
        for r in range(img_rows // strip):
            rows = slice(r * strip, (r + 1) * strip)
            sin_v, sin_before, turn, limit = sine[0, rows], sine[1, rows], sine[2, rows], sine[3, rows]
            for k, start in enumerate(starts):
                cols = slice(k * LANES, (k + 1) * LANES)
                noisy = jnp.where(term[k] < limit, sin_v, 0.0) * noise[k]
                pixels = img[rows, pl.ds(start, LANES)].astype(jnp.float32)
                weighted[slot, rows, cols] = (noisy * pixels).astype(jnp.bfloat16)
                weighted_sq[slot, rows, cols] = (noisy * (-0.5 * sin_v)).astype(jnp.bfloat16)
                sin_v, sin_before = turn * sin_v - sin_before, sin_v
            sine[0, rows] = sin_v
            sine[1, rows] = sin_before

    def score_chunk(c, slot):
        rows = proj[:, pl.ds(pl.multiple_of(c * DEPTH, DEPTH), DEPTH)]
        got = lax.dot_general(rows, weighted[slot], contract, preferred_element_type=jnp.float32)
        got = got + lax.dot_general(rows * rows, weighted_sq[slot], contract, preferred_element_type=jnp.float32)
        total[...] += got

    def move_img(t, n):
        rows = pl.ds(pl.multiple_of((side * PIECES + n) * piece, piece), piece)
        slab = pl.ds(pl.multiple_of(img_to(t) * part, LANES), part)
        return pltpu.make_async_remote_copy(
            src_ref=img_hbm.at[rows, slab], dst_ref=moved.at[t, rows, :], send_sem=img_send,
            recv_sem=img_recv.at[t - 2, n], device_id={"img": img_to(t)}, device_id_type=MESH)

    near = pltpu.make_async_remote_copy(
        src_ref=img_hbm.at[:, pl.ds(pl.multiple_of(img_to(1) * part, LANES), part)], dst_ref=moved.at[1],
        send_sem=near_sem.at[0], recv_sem=near_sem.at[1], device_id={"img": img_to(1)}, device_id_type=MESH)
    small = [pltpu.make_async_remote_copy(
        src_ref=ref, dst_ref=dst.at[t], send_sem=small_send.at[n], recv_sem=small_recv.at[n],
        device_id={"img": img_to(t)}, device_id_type=MESH)
        for t in range(1, n_img) for n, (ref, dst) in enumerate(((focus_ref, focus_all), (limit_ref, limit_all)))]
    far = [(t, n) for n in range(PIECES) for t in range(2, n_img)]

    with jax.named_scope("img0"):
        load_img(0).wait()
    terms_chunk(jnp.int32(0), 0)

    def score_step(i, carry):
        with jax.named_scope("loads"):
            load_proj(i).wait()
            pl.when(i + 1 < steps)(lambda: load_img(i + 1).wait())

        @pl.when(i == NEAR_STEP)
        def _():
            with jax.named_scope("near"):
                pl.semaphore_wait(barrier, n_img * x_size - 1 + jnp.where(bottom, 0, 1) + jnp.where(top, 0, 1))
            pl.when(bottom)(lambda: signal(up_token, me, mine + x_size))
            pl.when(top)(lambda: signal(down_token, me, mine - x_size))
            for copy in small:
                copy.start()
            for t, n in far:
                move_img(t, n).start()
            near.start()

        score_chunk(2 * i, 0)
        terms_chunk(2 * i + 1, 1)
        score_chunk(2 * i + 1, 1)
        terms_chunk(jnp.minimum(2 * i + 2, width // DEPTH - 1), 0)
        return carry

    lax.fori_loop(0, steps, score_step, 0)

    with jax.named_scope("smax"):
        small_loads[3].wait()
        small_loads[4].wait()
    scores = total[...]
    orient = lax.broadcasted_iota(jnp.int32, (proj_rows, img_rows), 0) + mine * proj_rows
    significant = orient < count_ref[...]
    masked = jnp.where(significant, scores, -1e30)
    peak = jnp.max(masked, axis=0, keepdims=True)
    expo = jnp.where(significant, jnp.exp(masked - peak), 0.0)
    stats[0:1, :] = peak
    stats[1:2, :] = jnp.sum(expo, axis=0, keepdims=True)
    terms[...] = expo.astype(jnp.bfloat16)

    def send_stat(k, carry):
        target, t = k // n_img, lax.rem(k, n_img)
        slot = t * n_proj + lax.rem(target - mine + n_proj, n_proj)

        @pl.when(slot > 0)
        def _():
            pltpu.make_async_remote_copy(
                src_ref=stats, dst_ref=every_stats.at[slot], send_sem=stat_send, recv_sem=stat_recv,
                device_id={"img": img_to(t), "proj": target}, device_id_type=MESH).start()
        return carry

    plane = x_size * n_img

    @pl.when(jnp.logical_not(bottom))
    def _():
        with jax.named_scope("up"):
            pl.semaphore_wait(up_token, 1)
        pl.when(jnp.logical_not(top))(lambda: signal(up_token, me, mine + x_size))

    with jax.named_scope("send"):
        lax.fori_loop(0, (at_z + 1) * plane, send_stat, 0)

    def learn_above():
        with jax.named_scope("down"):
            pl.semaphore_wait(down_token, 1)
        pl.when(jnp.logical_not(bottom))(lambda: signal(down_token, me, mine - x_size))
        lax.fori_loop((at_z + 1) * plane, z_size * plane, send_stat, 0)

    inner = jnp.logical_not(jnp.logical_or(bottom, top))
    pl.when(jnp.logical_and(inner, at_z == z_size - 2))(learn_above)

    post_copies = {t: pltpu.make_async_remote_copy(
        src_ref=terms, dst_ref=every_terms.at[t], send_sem=post_send, recv_sem=post_recv.at[t - 1],
        device_id={"img": img_to(t)}, device_id_type=MESH) for t in (1, *range(2, n_img, 2))}
    for t in range(2, n_img, 2):
        post_copies[t + 1] = pltpu.make_async_remote_copy(
            src_ref=every_terms.at[t], dst_ref=every_terms.at[t + 1], send_sem=post_send,
            recv_sem=post_recv.at[t], device_id={"img": img_to(1)}, device_id_type=MESH)
    for t in (*range(2, n_img, 2), 1):
        post_copies[t].start()

    term0 = lane + (me * part).astype(jnp.float32)

    def weights_block(t, carry):
        sine[0], sine[1], sine[2] = sine_start(focus_all[t], term0, width)
        sine[3] = columns_of(limit_all[t].astype(jnp.float32), img_rows)
        for r in range(img_rows // strip):
            inside = slice(r * strip, (r + 1) * strip)
            rows = pl.ds(pl.multiple_of(t * img_rows + r * strip, strip), strip)
            sin_v, sin_before, turn, limit = sine[0, inside], sine[1, inside], sine[2, inside], sine[3, inside]
            for c in range(part // LANES):
                cols = slice(c * LANES, (c + 1) * LANES)
                kept = jnp.where(term0 + float(c * LANES) < limit, sin_v, 0.0)
                contrast[rows, cols] = kept
                back_wgt[rows, cols] = (kept * sin_v).astype(jnp.bfloat16)
                sin_v, sin_before = turn * sin_v - sin_before, sin_v
        return carry

    def take_images(t, first, pixels):
        rows = pl.ds(pl.multiple_of(t * img_rows + first, piece), pixels.shape[0])
        back_img[rows, :] = (contrast[rows, :] * pixels.astype(jnp.float32)).astype(jnp.bfloat16)

    def take_piece(t, half, n):
        first = pl.multiple_of((half * PIECES + n) * piece, piece)
        take_images(t, first, moved[t, pl.ds(first, piece), :])

    passed = []

    def pass_on(t, n):
        with jax.named_scope(f"mv{t}{n}"):
            move_img(t, n).wait_recv()
        held = moved.at[t, pl.ds(pl.multiple_of((side * PIECES + n) * piece, piece), piece), :]
        passed.append(pltpu.make_async_remote_copy(
            src_ref=held, dst_ref=held, send_sem=pass_send, recv_sem=pass_recv.at[t - 2, n],
            device_id={"proj": across[n % 2]}, device_id_type=MESH))
        passed[-1].start()

    focus_all[0] = focus_ref[...]
    limit_all[0] = limit_ref[...]
    with jax.named_scope("smallx"):
        for n, every in enumerate((focus_all, limit_all)):
            wait_bytes(every.at[pl.ds(1, n_img - 1)], small_recv.at[n])
    per_piece = n_img - 2
    with jax.named_scope("weights"):
        lax.fori_loop(0, n_img // 2, weights_block, 0)
    for t, n in far[:per_piece]:
        pass_on(t, n)
    pl.when(jnp.logical_and(inner, at_z != z_size - 2))(learn_above)
    lax.fori_loop(n_img // 2, n_img, weights_block, 0)
    for t, n in far[per_piece:2 * per_piece]:
        pass_on(t, n)
    take_images(0, 0, img[:, pl.ds(pl.multiple_of(me * part, LANES), part)])
    with jax.named_scope("nearimg"):
        near.wait()
    take_images(1, 0, moved[1])
    pl.when(jnp.logical_and(bottom, jnp.logical_not(top)))(learn_above)
    for t, n in far[2 * per_piece:]:
        pass_on(t, n)
    for t in range(2, n_img, 2):
        with jax.named_scope(f"post{t}"):
            post_copies[t].wait_recv()
        post_copies[t + 1].start()
    for t, n in far:
        take_piece(t, side, n)

    every_stats[0] = stats[...]
    with jax.named_scope("stat"):
        wait_bytes(every_stats.at[pl.ds(1, n_img * n_proj - 1)], stat_recv)
    evidence = []
    for t in range(n_img):
        every = every_stats[pl.ds(t * n_proj, n_proj)]
        peaks, masses = every[:, 0, :], every[:, 1, :]
        highest = jnp.max(peaks, axis=0, keepdims=True)
        whole = jnp.sum(masses * jnp.exp(peaks - highest), axis=0, keepdims=True)
        evidence.append(highest + jnp.log(whole))
        scale = jnp.exp(peaks[0:1, :] - evidence[t])
        if t % 2:
            with jax.named_scope(f"post{t}"):
                post_copies[t].wait_recv()
        values = every_terms[t].astype(jnp.float32) if t else terms[...].astype(jnp.float32)
        posts_ref[:, t * img_rows:(t + 1) * img_rows] = (values * scale).astype(jnp.bfloat16)

    groups = img_rows // BLOCK
    group = lax.broadcasted_iota(jnp.int32, (1, img_rows), 1) // BLOCK
    placed = jnp.zeros((1, img_rows), jnp.float32)
    for t in range(n_img):
        plan = jnp.zeros((1, img_rows), jnp.int32)
        for g in range(groups):
            plan = jnp.where(group == g, plan_ref[img_from(t) * groups + g], plan)
        for s in range(groups):
            turned, target = evidence[t], plan
            if s:
                turned = pltpu.roll(evidence[t], s * BLOCK, 1)
                target = pltpu.roll(plan, s * BLOCK, 1)
            placed = placed + jnp.where(target == me * groups + group, turned, 0.0)
    ev_ref[...] = placed

    wait_bytes(every_stats.at[pl.ds(1, n_img * n_proj - 1)], stat_send)
    for n, every in enumerate((focus_all, limit_all)):
        wait_bytes(every.at[pl.ds(1, n_img - 1)], small_send.at[n])
    wait_bytes(every_terms.at[pl.ds(1, n_img - 1)], post_send)
    wait_bytes(moved.at[pl.ds(2, n_img - 2), pl.ds(0, img_rows // 2)], img_send)
    for q, (t, n) in enumerate(far):
        with jax.named_scope(f"ps{q}"):
            passed[q].wait_recv()
        take_piece(t, 1 - side, n)
    wait_bytes(moved.at[pl.ds(2, n_img - 2), pl.ds(0, img_rows // 2)], pass_send)


def back_kernel(posts_ref, back_img, back_wgt, ev_ref, rec_hbm, placed_hbm, rec, out_sem):
    part = back_img.shape[1]
    step = min(part, 256)
    steps = part // step
    posts = posts_ref[...]
    last = pltpu.make_async_copy(ev_ref, placed_hbm, out_sem.at[steps])
    last.start()
    copies = [last]
    for c in range(steps):
        cols = slice(c * step, (c + 1) * step)
        sums = jnp.dot(posts, back_img[:, cols], preferred_element_type=jnp.float32)
        weights = jnp.dot(posts, back_wgt[:, cols], preferred_element_type=jnp.float32)
        rec[:, cols] = (sums / (weights + 1.0)).astype(jnp.bfloat16)
        copies.append(pltpu.make_async_copy(rec.at[:, cols], rec_hbm.at[:, cols], out_sem.at[c]))
        copies[-1].start()
    for copy in copies:
        copy.wait()


def shards(n_img, n_proj, images, projections, noise_weight, defocus, orient_count, term_limit, block_plan):
    img_rows, width = images.shape
    proj_rows = projections.shape[0]
    part = width // n_img
    x_size = 1 << ((n_proj.bit_length() - 1) // 2)
    vmem = pl.BlockSpec(memory_space=pltpu.VMEM)
    hbm = pl.BlockSpec(memory_space=pl.ANY)
    bf16, f32, i32 = jnp.bfloat16, jnp.float32, jnp.int32
    dma, regular = pltpu.SemaphoreType.DMA, pltpu.SemaphoreType.REGULAR
    held = pl.pallas_call(
        functools.partial(score_kernel, n_img, n_proj, x_size),
        out_shape=(pltpu.VMEM((proj_rows, n_img * img_rows), bf16), pltpu.VMEM((n_img * img_rows, part), bf16),
                   pltpu.VMEM((n_img * img_rows, part), bf16), pltpu.VMEM((1, img_rows), f32)),
        in_specs=[hbm] * 7,
        out_specs=(vmem, vmem, vmem, vmem),
        scratch_shapes=[
            pltpu.VMEM((img_rows, width), bf16),
            pltpu.VMEM((proj_rows, width), bf16),
            pltpu.VMEM((1, width), f32),
            pltpu.VMEM((1, img_rows), f32),
            pltpu.VMEM((1, img_rows), i32),
            pltpu.VMEM((1, img_rows), i32),
            pltpu.SMEM(block_plan.shape, i32),
            pltpu.VMEM((2, img_rows, DEPTH), bf16),
            pltpu.VMEM((2, img_rows, DEPTH), bf16),
            pltpu.VMEM((proj_rows, img_rows), f32),
            pltpu.VMEM((4, img_rows, LANES), f32),
            pltpu.VMEM((n_img, img_rows, part), bf16),
            pltpu.VMEM((n_img * img_rows, part), f32),
            pltpu.VMEM((n_img, 1, img_rows), f32),
            pltpu.VMEM((n_img, 1, img_rows), i32),
            pltpu.VMEM((proj_rows, img_rows), bf16),
            pltpu.VMEM((n_img, proj_rows, img_rows), bf16),
            pltpu.VMEM((2, img_rows), f32),
            pltpu.VMEM((n_img * n_proj, 2, img_rows), f32),
            dma((5,)), dma((width // DEPTH // 2,)), dma((width // DEPTH // 2,)), regular, regular,
            dma((2,)), dma((2,)), dma((2,)), dma, dma((n_img - 2, PIECES)), dma, dma((n_img - 2, PIECES)),
            dma, dma((n_img - 1,)), dma, dma,
        ],
        compiler_params=pltpu.CompilerParams(
            collective_id=0, has_side_effects=True, vmem_limit_bytes=54 * 1024 * 1024),
    )(images, projections, noise_weight.reshape(1, -1), defocus.reshape(1, -1), orient_count.reshape(1, -1),
      term_limit.reshape(1, -1), block_plan)
    reconstruction, evidence = pl.pallas_call(
        back_kernel,
        out_shape=(jax.ShapeDtypeStruct((proj_rows, part), bf16), jax.ShapeDtypeStruct((1, img_rows), f32)),
        in_specs=[vmem] * 4,
        out_specs=(hbm, hbm),
        scratch_shapes=[pltpu.VMEM((proj_rows, part), bf16), dma((part // min(part, 256) + 1,))],
        compiler_params=pltpu.CompilerParams(vmem_limit_bytes=16 * 1024 * 1024),
    )(*held)
    return reconstruction, evidence.reshape(-1)


def solution(mesh):
    n_img, n_proj = mesh.shape["img"], mesh.shape["proj"]
    placed = (P("img", None), P("proj", None), P(), P("img"), P("img"), P("img"), P())
    return jax.shard_map(
        functools.partial(shards, n_img, n_proj), mesh=mesh, in_specs=placed,
        out_specs=(P("proj", "img"), P("img")), check_vma=False,
    )
```

```python
import functools
import math

import jax
import jax.numpy as jnp
from jax import lax
from jax.experimental import pallas as pl
from jax.experimental.pallas import tpu as pltpu
from jax.sharding import PartitionSpec as P

BLOCK = 32
PIECES = 2
PIECE = 16
LANES = 128
DEPTH = 512
NEAR_STEP = 1
MESH = pl.DeviceIdType.MESH
SIN_TERMS = [(-1.0) ** k * math.pi ** (2 * k + 1) / math.factorial(2 * k + 1) for k in range(7)]
COS_TERMS = [(-1.0) ** k * math.pi ** (2 * k) / math.factorial(2 * k) for k in range(8)]


def horner(terms, x):
    total = jnp.full_like(x, terms[-1])
    for term in terms[-2::-1]:
        total = total * x + term
    return total


def sincos_turns(turns):
    rest = turns - jnp.floor(turns + 0.5)
    square = rest * rest
    half_sin = rest * horner(SIN_TERMS, square)
    half_cos = horner(COS_TERMS, square)
    return 2.0 * half_sin * half_cos, 1.0 - 2.0 * half_sin * half_sin


def columns_of(row, rows):
    return jnp.broadcast_to(row, (LANES, rows)).T


def step_sines(row, width):
    sin_d, cos_d = sincos_turns(row * (LANES / width))
    rows = row.shape[1]
    return columns_of(sin_d, rows), columns_of(cos_d, rows)


def sine_start(row, term0, width):
    sin_d, cos_d = step_sines(row, width)
    focus = columns_of(row, row.shape[1])
    sin0, cos0 = sincos_turns(focus * ((term0 + 1.0) / width) + 0.1 / (2.0 * math.pi))
    return sin0, sin0 * cos_d - cos0 * sin_d, 2.0 * cos_d


def wait_bytes(ref, sem):
    pltpu.make_async_copy(ref, ref, sem).wait()


def score_kernel(n_img, n_proj, x_size, img_hbm, proj_hbm, noise_hbm, focus_hbm, count_hbm, limit_hbm, plan_hbm,
                 posts_ref, back_img, back_wgt, ev_ref,
                 img, proj, noise_ref, focus_ref, count_ref, limit_ref, plan_ref, weighted, weighted_sq, total,
                 sine, moved, contrast, focus_all, limit_all, terms, every_terms, stats, every_stats,
                 load_sem, img_load, proj_load, next_token, all_token,
                 small_send, small_recv, near_sem, img_send, img_recv, pass_send, pass_recv,
                 post_send, post_recv, stat_send, stat_recv):
    me = lax.axis_index("img")
    mine = lax.axis_index("proj")
    img_rows, width = img.shape
    proj_rows = proj.shape[0]
    part = width // n_img
    chips = n_img // 2
    row_y, core = me // 2, lax.rem(me, 2)
    at_x, at_z = lax.rem(mine, x_size), mine // x_size

    def img_to(t):
        return lax.rem(row_y + t // 2, chips) * 2 + lax.rem(core + lax.rem(t, 2), 2)

    def img_from(t):
        return lax.rem(row_y + chips - t // 2, chips) * 2 + lax.rem(core + t % 2, 2)

    odd_x, odd_z = lax.rem(at_x, 2), lax.rem(at_z, 2)
    side = lax.rem(odd_x + odd_z, 2)
    beside_x, beside_z = mine + 1 - 2 * odd_x, mine + x_size * (1 - 2 * odd_z)
    beside_xz = beside_x + beside_z - mine
    quarter = (img_rows - 2 * PIECES * PIECE) // 4

    def half_rows(k, n):
        return pl.ds(pl.multiple_of((k * PIECES + n) * PIECE, PIECE), PIECE)

    def quarter_rows(x, z):
        return pl.ds(pl.multiple_of(2 * PIECES * PIECE + (x * 2 + z) * quarter, 8), quarter)

    def signal(sem, img, proj):
        pl.semaphore_signal(sem, inc=1, device_id={"img": img, "proj": proj}, device_id_type=MESH)

    barrier = pltpu.get_barrier_semaphore()
    partner, first_core = img_to(1), core == 0

    def greet_next(t, proj):
        signal(barrier, img_to(t) - lax.rem(img_to(t), 2), proj)

    for k in range(1, x_size):
        greet_next(0, at_z * x_size + lax.rem(at_x + k, x_size))
    for t in range(2, n_img, 2):
        greet_next(t, mine)
    pl.when(jnp.logical_not(first_core))(lambda: signal(barrier, partner, mine))

    def greet_all(k, carry):
        chip, proj = k // n_proj, lax.rem(k, n_proj)
        row = chip * 2 + 1
        pl.when(jnp.logical_or(row != me, proj != mine))(lambda: signal(barrier, row, proj))
        return carry

    def meet_next():
        with jax.named_scope("near"):
            @pl.when(first_core)
            def _():
                pl.semaphore_wait(barrier, 2 * (chips - 1) + 2 * (x_size - 1) + 1)
                signal(next_token, partner, mine)
            pl.when(jnp.logical_not(first_core))(lambda: pl.semaphore_wait(next_token, 1))

    def meet_all():
        with jax.named_scope("all"):
            @pl.when(jnp.logical_not(first_core))
            def _():
                pl.semaphore_wait(barrier, n_img * n_proj - 1)
                signal(all_token, partner, mine)
            pl.when(first_core)(lambda: pl.semaphore_wait(all_token, 1))

    small_loads = [pltpu.make_async_copy(source, target, load_sem.at[n]) for n, (source, target) in enumerate(
        ((focus_hbm, focus_ref), (limit_hbm, limit_ref), (noise_hbm, noise_ref), (count_hbm, count_ref),
         (plan_hbm, plan_ref)))]
    wide = 2 * DEPTH
    steps = width // wide

    def load_img(n):
        cols = pl.ds(pl.multiple_of(n * wide, wide), wide)
        return pltpu.make_async_copy(img_hbm.at[:, cols], img.at[:, cols], img_load.at[n])

    def load_proj(n):
        cols = pl.ds(pl.multiple_of(n * wide, wide), wide)
        return pltpu.make_async_copy(proj_hbm.at[:, cols], proj.at[:, cols], proj_load.at[n])

    for load in small_loads[:3]:
        load.start()
    load_img(0).start()
    for n in range(steps):
        load_proj(n).start()
        if n + 1 < steps:
            load_img(n + 1).start()
    for load in small_loads[3:]:
        load.start()
    lax.fori_loop(0, chips * n_proj, greet_all, 0)
    with jax.named_scope("small"):
        small_loads[0].wait()
        small_loads[1].wait()

    lane = lax.broadcasted_iota(jnp.int32, (1, LANES), 1).astype(jnp.float32)
    sine[0], sine[1], sine[2] = sine_start(focus_ref[...], lane, width)
    sine[3] = columns_of(limit_ref[...].astype(jnp.float32), img_rows)
    total[...] = jnp.zeros_like(total)
    small_loads[2].wait()
    contract = (((1,), (1,)), ((), ()))
    strip = 16

    def terms_chunk(c, slot):
        starts = [pl.multiple_of(c * DEPTH + k * LANES, LANES) for k in range(DEPTH // LANES)]
        noise = [noise_ref[:, pl.ds(start, LANES)] for start in starts]
        term = [lane + start.astype(jnp.float32) for start in starts]
        for r in range(img_rows // strip):
            rows = slice(r * strip, (r + 1) * strip)
            sin_v, sin_before, turn, limit = sine[0, rows], sine[1, rows], sine[2, rows], sine[3, rows]
            for k, start in enumerate(starts):
                cols = slice(k * LANES, (k + 1) * LANES)
                noisy = jnp.where(term[k] < limit, sin_v, 0.0) * noise[k]
                pixels = img[rows, pl.ds(start, LANES)].astype(jnp.float32)
                weighted[slot, rows, cols] = (noisy * pixels).astype(jnp.bfloat16)
                weighted_sq[slot, rows, cols] = (noisy * (-0.5 * sin_v)).astype(jnp.bfloat16)
                sin_v, sin_before = turn * sin_v - sin_before, sin_v
            sine[0, rows] = sin_v
            sine[1, rows] = sin_before

    def score_chunk(c, slot):
        rows = proj[:, pl.ds(pl.multiple_of(c * DEPTH, DEPTH), DEPTH)]
        got = lax.dot_general(rows, weighted[slot], contract, preferred_element_type=jnp.float32)
        got = got + lax.dot_general(rows * rows, weighted_sq[slot], contract, preferred_element_type=jnp.float32)
        total[...] += got

    my_rows = [quarter_rows(odd_x, odd_z)] + [half_rows(side, n) for n in range(PIECES)]

    def move_img(t, n):
        slab = pl.ds(pl.multiple_of(img_to(t) * part, LANES), part)
        return pltpu.make_async_remote_copy(
            src_ref=img_hbm.at[my_rows[n], slab], dst_ref=moved.at[t, my_rows[n], :], send_sem=img_send,
            recv_sem=img_recv.at[t - 2, n], device_id={"img": img_to(t)}, device_id_type=MESH)

    def pass_rows(t, rows, proj):
        held = moved.at[t, rows, :]
        pltpu.make_async_remote_copy(
            src_ref=held, dst_ref=held, send_sem=pass_send, recv_sem=pass_recv, device_id={"proj": proj},
            device_id_type=MESH).start()

    near = pltpu.make_async_remote_copy(
        src_ref=img_hbm.at[:, pl.ds(pl.multiple_of(img_to(1) * part, LANES), part)], dst_ref=moved.at[1],
        send_sem=near_sem.at[0], recv_sem=near_sem.at[1], device_id={"img": img_to(1)}, device_id_type=MESH)
    small = [pltpu.make_async_remote_copy(
        src_ref=ref, dst_ref=dst.at[t], send_sem=small_send.at[n], recv_sem=small_recv.at[n],
        device_id={"img": img_to(t)}, device_id_type=MESH)
        for t in range(1, n_img) for n, (ref, dst) in enumerate(((focus_ref, focus_all), (limit_ref, limit_all)))]
    far = [(t, n) for n in range(PIECES + 1) for t in range(2, n_img)]

    with jax.named_scope("img0"):
        load_img(0).wait()
    terms_chunk(jnp.int32(0), 0)

    def score_step(i, carry):
        with jax.named_scope("loads"):
            load_proj(i).wait()
            pl.when(i + 1 < steps)(lambda: load_img(i + 1).wait())

        @pl.when(i == NEAR_STEP)
        def _():
            meet_next()
            for copy in small:
                copy.start()
            for t, n in far:
                move_img(t, n).start()
            near.start()

        score_chunk(2 * i, 0)
        terms_chunk(2 * i + 1, 1)
        score_chunk(2 * i + 1, 1)
        terms_chunk(jnp.minimum(2 * i + 2, width // DEPTH - 1), 0)
        return carry

    lax.fori_loop(0, steps, score_step, 0)

    with jax.named_scope("smax"):
        small_loads[3].wait()
        small_loads[4].wait()
    scores = total[...]
    orient = lax.broadcasted_iota(jnp.int32, (proj_rows, img_rows), 0) + mine * proj_rows
    significant = orient < count_ref[...]
    masked = jnp.where(significant, scores, -1e30)
    peak = jnp.max(masked, axis=0, keepdims=True)
    expo = jnp.where(significant, jnp.exp(masked - peak), 0.0)
    stats[0:1, :] = peak
    stats[1:2, :] = jnp.sum(expo, axis=0, keepdims=True)
    terms[...] = expo.astype(jnp.bfloat16)

    def send_stat(k, carry):
        target, t = k // n_img, lax.rem(k, n_img)
        slot = t * n_proj + lax.rem(target - mine + n_proj, n_proj)

        @pl.when(slot > 0)
        def _():
            pltpu.make_async_remote_copy(
                src_ref=stats, dst_ref=every_stats.at[slot], send_sem=stat_send, recv_sem=stat_recv,
                device_id={"img": img_to(t), "proj": target}, device_id_type=MESH).start()
        return carry

    meet_all()
    with jax.named_scope("send"):
        lax.fori_loop(0, n_img * n_proj, send_stat, 0)

    post_copies = {t: pltpu.make_async_remote_copy(
        src_ref=terms, dst_ref=every_terms.at[t], send_sem=post_send, recv_sem=post_recv.at[t - 1],
        device_id={"img": img_to(t)}, device_id_type=MESH) for t in (1, *range(2, n_img, 2))}
    for t in range(2, n_img, 2):
        post_copies[t + 1] = pltpu.make_async_remote_copy(
            src_ref=every_terms.at[t], dst_ref=every_terms.at[t + 1], send_sem=post_send,
            recv_sem=post_recv.at[t], device_id={"img": img_to(1)}, device_id_type=MESH)
    post_copies[1].start()

    term0 = lane + (me * part).astype(jnp.float32)

    def weights_block(t, carry):
        sine[0], sine[1], sine[2] = sine_start(focus_all[t], term0, width)
        sine[3] = columns_of(limit_all[t].astype(jnp.float32), img_rows)
        for r in range(img_rows // strip):
            inside = slice(r * strip, (r + 1) * strip)
            rows = pl.ds(pl.multiple_of(t * img_rows + r * strip, strip), strip)
            sin_v, sin_before, turn, limit = sine[0, inside], sine[1, inside], sine[2, inside], sine[3, inside]
            for c in range(part // LANES):
                cols = slice(c * LANES, (c + 1) * LANES)
                kept = jnp.where(term0 + float(c * LANES) < limit, sin_v, 0.0)
                contrast[rows, cols] = kept
                back_wgt[rows, cols] = (kept * sin_v).astype(jnp.bfloat16)
                sin_v, sin_before = turn * sin_v - sin_before, sin_v
        return carry

    def take_images(t, first, pixels):
        rows = pl.ds(pl.multiple_of(t * img_rows + first, 8), pixels.shape[0])
        back_img[rows, :] = (contrast[rows, :] * pixels.astype(jnp.float32)).astype(jnp.bfloat16)

    def take_rows(t, rows):
        take_images(t, rows.start, moved[t, rows, :])

    def pass_on(t, n):
        with jax.named_scope(f"mv{t}{n}"):
            move_img(t, n).wait_recv()
        if n:
            pass_rows(t, my_rows[n], (beside_x, beside_z)[(n + t) % 2])
        else:
            for proj in (beside_xz, beside_x, beside_z):
                pass_rows(t, my_rows[0], proj)

    other_rows = [quarter_rows(1 - odd_x, odd_z), quarter_rows(odd_x, 1 - odd_z), quarter_rows(1 - odd_x, 1 - odd_z)]
    other_rows += [half_rows(1 - side, n) for n in range(PIECES)]

    focus_all[0] = focus_ref[...]
    limit_all[0] = limit_ref[...]
    fill_weights = lambda lo, hi: lax.fori_loop(lo, hi, weights_block, 0)
    fill_weights(0, 1)
    with jax.named_scope("smallx"):
        for n, every in enumerate((focus_all, limit_all)):
            wait_bytes(every.at[pl.ds(1, n_img - 1)], small_recv.at[n])
    per_piece = n_img - 2
    fill_weights(1, 2)
    for t, n in far[:per_piece]:
        pass_on(t, n)
    fill_weights(2, 2 + per_piece // 2)
    for t, n in far[per_piece:2 * per_piece]:
        pass_on(t, n)
    for t in range(2, n_img, 2):
        post_copies[t].start()
    fill_weights(2 + per_piece // 2, n_img)
    take_images(0, 0, img[:, pl.ds(pl.multiple_of(me * part, LANES), part)])
    with jax.named_scope("nearimg"):
        near.wait()
    take_images(1, 0, moved[1])
    for t, n in far[2 * per_piece:]:
        pass_on(t, n)
    for t in range(2, n_img, 2):
        with jax.named_scope(f"post{t}"):
            post_copies[t].wait_recv()
        post_copies[t + 1].start()
    for t, n in far:
        take_rows(t, my_rows[n])

    every_stats[0] = stats[...]
    with jax.named_scope("stat"):
        wait_bytes(every_stats.at[pl.ds(1, n_img * n_proj - 1)], stat_recv)
    evidence = []
    for t in range(n_img):
        every = every_stats[pl.ds(t * n_proj, n_proj)]
        peaks, masses = every[:, 0, :], every[:, 1, :]
        highest = jnp.max(peaks, axis=0, keepdims=True)
        whole = jnp.sum(masses * jnp.exp(peaks - highest), axis=0, keepdims=True)
        evidence.append(highest + jnp.log(whole))
        scale = jnp.exp(peaks[0:1, :] - evidence[t])
        if t % 2:
            with jax.named_scope(f"post{t}"):
                post_copies[t].wait_recv()
        values = every_terms[t].astype(jnp.float32) if t else terms[...].astype(jnp.float32)
        posts_ref[:, t * img_rows:(t + 1) * img_rows] = (values * scale).astype(jnp.bfloat16)

    groups = img_rows // BLOCK
    group = lax.broadcasted_iota(jnp.int32, (1, img_rows), 1) // BLOCK
    placed = jnp.zeros((1, img_rows), jnp.float32)
    for t in range(n_img):
        plan = jnp.zeros((1, img_rows), jnp.int32)
        for g in range(groups):
            plan = jnp.where(group == g, plan_ref[img_from(t) * groups + g], plan)
        for s in range(groups):
            turned, target = evidence[t], plan
            if s:
                turned = pltpu.roll(evidence[t], s * BLOCK, 1)
                target = pltpu.roll(plan, s * BLOCK, 1)
            placed = placed + jnp.where(target == me * groups + group, turned, 0.0)
    ev_ref[...] = placed

    wait_bytes(every_stats.at[pl.ds(1, n_img * n_proj - 1)], stat_send)
    for n, every in enumerate((focus_all, limit_all)):
        wait_bytes(every.at[pl.ds(1, n_img - 1)], small_send.at[n])
    wait_bytes(every_terms.at[pl.ds(1, n_img - 1)], post_send)
    sent, handed = PIECES * PIECE + quarter, PIECES * PIECE + 3 * quarter
    wait_bytes(moved.at[pl.ds(2, n_img - 2), pl.ds(0, sent)], img_send)
    handed_rows = moved.at[pl.ds(2, n_img - 2), pl.ds(0, handed)]
    with jax.named_scope("pass"):
        wait_bytes(handed_rows, pass_recv)
    for t in range(2, n_img):
        for rows in other_rows:
            take_rows(t, rows)
    wait_bytes(handed_rows, pass_send)


def back_kernel(posts_ref, back_img, back_wgt, ev_ref, rec_hbm, placed_hbm, rec, out_sem):
    part = back_img.shape[1]
    step = min(part, 256)
    steps = part // step
    posts = posts_ref[...]
    last = pltpu.make_async_copy(ev_ref, placed_hbm, out_sem.at[steps])
    last.start()
    copies = [last]
    for c in range(steps):
        cols = slice(c * step, (c + 1) * step)
        sums = jnp.dot(posts, back_img[:, cols], preferred_element_type=jnp.float32)
        weights = jnp.dot(posts, back_wgt[:, cols], preferred_element_type=jnp.float32)
        rec[:, cols] = (sums / (weights + 1.0)).astype(jnp.bfloat16)
        copies.append(pltpu.make_async_copy(rec.at[:, cols], rec_hbm.at[:, cols], out_sem.at[c]))
        copies[-1].start()
    for copy in copies:
        copy.wait()


def shards(n_img, n_proj, images, projections, noise_weight, defocus, orient_count, term_limit, block_plan):
    img_rows, width = images.shape
    proj_rows = projections.shape[0]
    part = width // n_img
    x_size = 1 << ((n_proj.bit_length() - 1) // 2)
    vmem = pl.BlockSpec(memory_space=pltpu.VMEM)
    hbm = pl.BlockSpec(memory_space=pl.ANY)
    bf16, f32, i32 = jnp.bfloat16, jnp.float32, jnp.int32
    dma, regular = pltpu.SemaphoreType.DMA, pltpu.SemaphoreType.REGULAR
    held = pl.pallas_call(
        functools.partial(score_kernel, n_img, n_proj, x_size),
        out_shape=(pltpu.VMEM((proj_rows, n_img * img_rows), bf16), pltpu.VMEM((n_img * img_rows, part), bf16),
                   pltpu.VMEM((n_img * img_rows, part), bf16), pltpu.VMEM((1, img_rows), f32)),
        in_specs=[hbm] * 7,
        out_specs=(vmem, vmem, vmem, vmem),
        scratch_shapes=[
            pltpu.VMEM((img_rows, width), bf16),
            pltpu.VMEM((proj_rows, width), bf16),
            pltpu.VMEM((1, width), f32),
            pltpu.VMEM((1, img_rows), f32),
            pltpu.VMEM((1, img_rows), i32),
            pltpu.VMEM((1, img_rows), i32),
            pltpu.SMEM(block_plan.shape, i32),
            pltpu.VMEM((2, img_rows, DEPTH), bf16),
            pltpu.VMEM((2, img_rows, DEPTH), bf16),
            pltpu.VMEM((proj_rows, img_rows), f32),
            pltpu.VMEM((4, img_rows, LANES), f32),
            pltpu.VMEM((n_img, img_rows, part), bf16),
            pltpu.VMEM((n_img * img_rows, part), f32),
            pltpu.VMEM((n_img, 1, img_rows), f32),
            pltpu.VMEM((n_img, 1, img_rows), i32),
            pltpu.VMEM((proj_rows, img_rows), bf16),
            pltpu.VMEM((n_img, proj_rows, img_rows), bf16),
            pltpu.VMEM((2, img_rows), f32),
            pltpu.VMEM((n_img * n_proj, 2, img_rows), f32),
            dma((5,)), dma((width // DEPTH // 2,)), dma((width // DEPTH // 2,)), regular, regular,
            dma((2,)), dma((2,)), dma((2,)), dma, dma((n_img - 2, PIECES + 1)), dma, dma,
            dma, dma((n_img - 1,)), dma, dma,
        ],
        compiler_params=pltpu.CompilerParams(
            collective_id=0, has_side_effects=True, vmem_limit_bytes=54 * 1024 * 1024),
    )(images, projections, noise_weight.reshape(1, -1), defocus.reshape(1, -1), orient_count.reshape(1, -1),
      term_limit.reshape(1, -1), block_plan)
    reconstruction, evidence = pl.pallas_call(
        back_kernel,
        out_shape=(jax.ShapeDtypeStruct((proj_rows, part), bf16), jax.ShapeDtypeStruct((1, img_rows), f32)),
        in_specs=[vmem] * 4,
        out_specs=(hbm, hbm),
        scratch_shapes=[pltpu.VMEM((proj_rows, part), bf16), dma((part // min(part, 256) + 1,))],
        compiler_params=pltpu.CompilerParams(vmem_limit_bytes=16 * 1024 * 1024),
    )(*held)
    return reconstruction, evidence.reshape(-1)


def solution(mesh):
    n_img, n_proj = mesh.shape["img"], mesh.shape["proj"]
    placed = (P("img", None), P("proj", None), P(), P("img"), P("img"), P("img"), P())
    return jax.shard_map(
        functools.partial(shards, n_img, n_proj), mesh=mesh, in_specs=placed,
        out_specs=(P("proj", "img"), P("img")), check_vma=False,
    )
```

```python
import functools
import math

import jax
import jax.numpy as jnp
from jax import lax
from jax.experimental import pallas as pl
from jax.experimental.pallas import tpu as pltpu
from jax.sharding import PartitionSpec as P

BLOCK = 32
PIECES = 2
PIECE = 16
LANES = 128
DEPTH = 512
MESH = pl.DeviceIdType.MESH
SIN_TERMS = [(-1.0) ** k * math.pi ** (2 * k + 1) / math.factorial(2 * k + 1) for k in range(7)]
COS_TERMS = [(-1.0) ** k * math.pi ** (2 * k) / math.factorial(2 * k) for k in range(8)]


def horner(terms, x):
    total = jnp.full_like(x, terms[-1])
    for term in terms[-2::-1]:
        total = total * x + term
    return total


def sincos_turns(turns):
    rest = turns - jnp.floor(turns + 0.5)
    square = rest * rest
    half_sin = rest * horner(SIN_TERMS, square)
    half_cos = horner(COS_TERMS, square)
    return 2.0 * half_sin * half_cos, 1.0 - 2.0 * half_sin * half_sin


def columns_of(row, rows):
    return jnp.broadcast_to(row, (LANES, rows)).T


def step_sines(row, width):
    sin_d, cos_d = sincos_turns(row * (LANES / width))
    rows = row.shape[1]
    return columns_of(sin_d, rows), columns_of(cos_d, rows)


def sine_start(row, term0, width):
    sin_d, cos_d = step_sines(row, width)
    focus = columns_of(row, row.shape[1])
    sin0, cos0 = sincos_turns(focus * ((term0 + 1.0) / width) + 0.1 / (2.0 * math.pi))
    return sin0, sin0 * cos_d - cos0 * sin_d, 2.0 * cos_d


def wait_bytes(ref, sem):
    pltpu.make_async_copy(ref, ref, sem).wait()


def score_kernel(n_img, n_proj, x_size, img_hbm, proj_hbm, noise_hbm, focus_hbm, count_hbm, limit_hbm, plan_hbm,
                 posts_ref, back_img, back_wgt, ev_ref,
                 img, proj, noise_ref, focus_ref, count_ref, limit_ref, plan_ref, weighted, weighted_sq, total,
                 sine, moved, contrast, focus_all, limit_all, terms, every_terms, stats, every_stats,
                 load_sem, img_load, proj_load, next_token, all_token,
                 small_send, small_recv, near_sem, img_send, img_recv, pass_send, pass_recv,
                 post_send, post_recv, stat_send, stat_recv):
    me = lax.axis_index("img")
    mine = lax.axis_index("proj")
    img_rows, width = img.shape
    proj_rows = proj.shape[0]
    part = width // n_img
    chips = n_img // 2
    row_y, core = me // 2, lax.rem(me, 2)
    at_x, at_z = lax.rem(mine, x_size), mine // x_size

    def img_to(t):
        return lax.rem(row_y + t // 2, chips) * 2 + lax.rem(core + lax.rem(t, 2), 2)

    def img_from(t):
        return lax.rem(row_y + chips - t // 2, chips) * 2 + lax.rem(core + t % 2, 2)

    odd_x, odd_z = lax.rem(at_x, 2), lax.rem(at_z, 2)
    side = lax.rem(odd_x + odd_z, 2)
    beside_x, beside_z = mine + 1 - 2 * odd_x, mine + x_size * (1 - 2 * odd_z)
    beside_xz = beside_x + beside_z - mine
    quarter = (img_rows - 2 * PIECES * PIECE) // 4

    def half_rows(k, n):
        return pl.ds(pl.multiple_of((k * PIECES + n) * PIECE, PIECE), PIECE)

    def quarter_rows(x, z):
        return pl.ds(pl.multiple_of(2 * PIECES * PIECE + (x * 2 + z) * quarter, 8), quarter)

    def signal(sem, img, proj):
        pl.semaphore_signal(sem, inc=1, device_id={"img": img, "proj": proj}, device_id_type=MESH)

    barrier = pltpu.get_barrier_semaphore()
    partner, first_core = img_to(1), core == 0

    def greet_next(t, proj):
        signal(barrier, img_to(t) - lax.rem(img_to(t), 2), proj)

    for k in range(1, x_size):
        greet_next(0, at_z * x_size + lax.rem(at_x + k, x_size))
    for t in range(2, n_img, 2):
        greet_next(t, mine)
    pl.when(jnp.logical_not(first_core))(lambda: signal(barrier, partner, mine))

    def greet_all(proj, carry):
        for chip in range(chips):
            pl.when(jnp.logical_or(chip * 2 + 1 != me, proj != mine))(lambda: signal(barrier, chip * 2 + 1, proj))
        return carry

    def meet_all():
        with jax.named_scope("all"):
            @pl.when(jnp.logical_not(first_core))
            def _():
                pl.semaphore_wait(barrier, n_img * n_proj - 1)
                signal(all_token, partner, mine)
            pl.when(first_core)(lambda: pl.semaphore_wait(all_token, 1))

    small_loads = [pltpu.make_async_copy(source, target, load_sem.at[n]) for n, (source, target) in enumerate(
        ((focus_hbm, focus_ref), (limit_hbm, limit_ref), (noise_hbm, noise_ref), (count_hbm, count_ref),
         (plan_hbm, plan_ref)))]
    wide = 2 * DEPTH
    steps = width // wide

    def load_img(n):
        cols = pl.ds(pl.multiple_of(n * wide, wide), wide)
        return pltpu.make_async_copy(img_hbm.at[:, cols], img.at[:, cols], img_load.at[n])

    def load_proj(n):
        cols = pl.ds(pl.multiple_of(n * wide, wide), wide)
        return pltpu.make_async_copy(proj_hbm.at[:, cols], proj.at[:, cols], proj_load.at[n])

    for load in small_loads[:3]:
        load.start()
    load_img(0).start()
    for n in range(steps):
        load_proj(n).start()
        if n + 1 < steps:
            load_img(n + 1).start()
    for load in small_loads[3:]:
        load.start()
    with jax.named_scope('greet'):
        lax.fori_loop(0, n_proj, greet_all, 0)
    my_rows = [quarter_rows(odd_x, odd_z)] + [half_rows(side, n) for n in range(PIECES)]

    def move_img(t, n):
        slab = pl.ds(pl.multiple_of(img_to(t) * part, LANES), part)
        return pltpu.make_async_remote_copy(
            src_ref=img_hbm.at[my_rows[n], slab], dst_ref=moved.at[t, my_rows[n], :], send_sem=img_send,
            recv_sem=img_recv.at[t - 2, n], device_id={"img": img_to(t)}, device_id_type=MESH)

    def pass_rows(t, rows, proj):
        held = moved.at[t, rows, :]
        pltpu.make_async_remote_copy(
            src_ref=held, dst_ref=held, send_sem=pass_send, recv_sem=pass_recv, device_id={"proj": proj},
            device_id_type=MESH).start()

    near = pltpu.make_async_remote_copy(
        src_ref=img_hbm.at[:, pl.ds(pl.multiple_of(img_to(1) * part, LANES), part)], dst_ref=moved.at[1],
        send_sem=near_sem.at[0], recv_sem=near_sem.at[1], device_id={"img": img_to(1)}, device_id_type=MESH)
    small = [pltpu.make_async_remote_copy(
        src_ref=ref, dst_ref=dst.at[t], send_sem=small_send.at[n], recv_sem=small_recv.at[n],
        device_id={"img": img_to(t)}, device_id_type=MESH)
        for t in range(1, n_img) for n, (ref, dst) in enumerate(((focus_hbm, focus_all), (limit_hbm, limit_all)))]
    far = [(t, n) for n in range(PIECES + 1) for t in range(2, n_img)]

    def send_images():
        for copy in small:
            copy.start()
        for t, n in far:
            move_img(t, n).start()
        near.start()

    @pl.when(first_core)
    def _():
        with jax.named_scope("near"):
            pl.semaphore_wait(barrier, 2 * (chips - 1) + 2 * (x_size - 1) + 1)
        signal(next_token, partner, mine)
        send_images()

    with jax.named_scope("small"):
        small_loads[0].wait()
        small_loads[1].wait()

    lane = lax.broadcasted_iota(jnp.int32, (1, LANES), 1).astype(jnp.float32)
    sine[0], sine[1], sine[2] = sine_start(focus_ref[...], lane, width)
    sine[3] = columns_of(limit_ref[...].astype(jnp.float32), img_rows)
    total[...] = jnp.zeros_like(total)
    small_loads[2].wait()
    contract = (((1,), (1,)), ((), ()))
    strip = 16

    def terms_chunk(c, slot):
        starts = [pl.multiple_of(c * DEPTH + k * LANES, LANES) for k in range(DEPTH // LANES)]
        noise = [noise_ref[:, pl.ds(start, LANES)] for start in starts]
        term = [lane + start.astype(jnp.float32) for start in starts]
        for r in range(img_rows // strip):
            rows = slice(r * strip, (r + 1) * strip)
            sin_v, sin_before, turn, limit = sine[0, rows], sine[1, rows], sine[2, rows], sine[3, rows]
            for k, start in enumerate(starts):
                cols = slice(k * LANES, (k + 1) * LANES)
                noisy = jnp.where(term[k] < limit, sin_v, 0.0) * noise[k]
                pixels = img[rows, pl.ds(start, LANES)].astype(jnp.float32)
                weighted[slot, rows, cols] = (noisy * pixels).astype(jnp.bfloat16)
                weighted_sq[slot, rows, cols] = (noisy * (-0.5 * sin_v)).astype(jnp.bfloat16)
                sin_v, sin_before = turn * sin_v - sin_before, sin_v
            sine[0, rows] = sin_v
            sine[1, rows] = sin_before

    def score_chunk(c, slot):
        rows = proj[:, pl.ds(pl.multiple_of(c * DEPTH, DEPTH), DEPTH)]
        got = lax.dot_general(rows, weighted[slot], contract, preferred_element_type=jnp.float32)
        got = got + lax.dot_general(rows * rows, weighted_sq[slot], contract, preferred_element_type=jnp.float32)
        total[...] += got

    with jax.named_scope("img0"):
        load_img(0).wait()
    terms_chunk(jnp.int32(0), 0)

    def score_step(i, carry):
        with jax.named_scope("loads"):
            load_proj(i).wait()
            pl.when(i + 1 < steps)(lambda: load_img(i + 1).wait())

        @pl.when(jnp.logical_and(i == 0, jnp.logical_not(first_core)))
        def _():
            with jax.named_scope("near"):
                pl.semaphore_wait(next_token, 1)
            send_images()

        score_chunk(2 * i, 0)
        terms_chunk(2 * i + 1, 1)
        score_chunk(2 * i + 1, 1)
        terms_chunk(jnp.minimum(2 * i + 2, width // DEPTH - 1), 0)
        return carry

    lax.fori_loop(0, steps, score_step, 0)

    with jax.named_scope("smax"):
        small_loads[3].wait()
        small_loads[4].wait()
    scores = total[...]
    orient = lax.broadcasted_iota(jnp.int32, (proj_rows, img_rows), 0) + mine * proj_rows
    significant = orient < count_ref[...]
    masked = jnp.where(significant, scores, -1e30)
    peak = jnp.max(masked, axis=0, keepdims=True)
    expo = jnp.where(significant, jnp.exp(masked - peak), 0.0)
    stats[0:1, :] = peak
    stats[1:2, :] = jnp.sum(expo, axis=0, keepdims=True)
    terms[...] = expo.astype(jnp.bfloat16)

    rows_of = [img_to(t) for t in range(n_img)]

    def send_stats(target, carry):
        ahead = target - mine
        ahead = jnp.where(ahead < 0, ahead + n_proj, ahead)
        for t in range(n_img):
            copy = pltpu.make_async_remote_copy(
                src_ref=stats, dst_ref=every_stats.at[t * n_proj + ahead], send_sem=stat_send, recv_sem=stat_recv,
                device_id={"img": rows_of[t], "proj": target}, device_id_type=MESH)
            if t:
                copy.start()
            else:
                pl.when(target != mine)(copy.start)
        return carry

    def pass_on(t, n):
        with jax.named_scope(f"mv{t}{n}"):
            move_img(t, n).wait_recv()
        if n:
            pass_rows(t, my_rows[n], (beside_x, beside_z)[(n + t) % 2])
        else:
            for proj in (beside_xz, beside_x, beside_z):
                pass_rows(t, my_rows[0], proj)

    meet_all()
    with jax.named_scope("send"):
        lax.fori_loop(0, n_proj, send_stats, 0)
    per_piece = n_img - 2
    for t, n in far[:per_piece]:
        pass_on(t, n)

    post_copies = {t: pltpu.make_async_remote_copy(
        src_ref=terms, dst_ref=every_terms.at[t], send_sem=post_send, recv_sem=post_recv.at[t - 1],
        device_id={"img": img_to(t)}, device_id_type=MESH) for t in (1, *range(2, n_img, 2))}
    for t in range(2, n_img, 2):
        post_copies[t + 1] = pltpu.make_async_remote_copy(
            src_ref=every_terms.at[t], dst_ref=every_terms.at[t + 1], send_sem=post_send,
            recv_sem=post_recv.at[t], device_id={"img": img_to(1)}, device_id_type=MESH)
    post_copies[1].start()
    for t in range(2, n_img, 2):
        post_copies[t].start()

    term0 = lane + (me * part).astype(jnp.float32)

    def weights_block(t, carry):
        sine[0], sine[1], sine[2] = sine_start(focus_all[t], term0, width)
        sine[3] = columns_of(limit_all[t].astype(jnp.float32), img_rows)
        for r in range(img_rows // strip):
            inside = slice(r * strip, (r + 1) * strip)
            rows = pl.ds(pl.multiple_of(t * img_rows + r * strip, strip), strip)
            sin_v, sin_before, turn, limit = sine[0, inside], sine[1, inside], sine[2, inside], sine[3, inside]
            for c in range(part // LANES):
                cols = slice(c * LANES, (c + 1) * LANES)
                kept = jnp.where(term0 + float(c * LANES) < limit, sin_v, 0.0)
                contrast[rows, cols] = kept
                back_wgt[rows, cols] = (kept * sin_v).astype(jnp.bfloat16)
                sin_v, sin_before = turn * sin_v - sin_before, sin_v
        return carry

    def take_images(t, first, pixels):
        rows = pl.ds(pl.multiple_of(t * img_rows + first, 8), pixels.shape[0])
        back_img[rows, :] = (contrast[rows, :] * pixels.astype(jnp.float32)).astype(jnp.bfloat16)

    def take_rows(t, rows):
        take_images(t, rows.start, moved[t, rows, :])

    other_rows = [quarter_rows(1 - odd_x, odd_z), quarter_rows(odd_x, 1 - odd_z), quarter_rows(1 - odd_x, 1 - odd_z)]
    other_rows += [half_rows(1 - side, n) for n in range(PIECES)]

    focus_all[0] = focus_ref[...]
    limit_all[0] = limit_ref[...]
    fill_weights = lambda lo, hi: lax.fori_loop(lo, hi, weights_block, 0)
    fill_weights(0, 1)
    with jax.named_scope("smallx"):
        for n, every in enumerate((focus_all, limit_all)):
            wait_bytes(every.at[pl.ds(1, n_img - 1)], small_recv.at[n])
    fill_weights(1, 2)
    fill_weights(2, 2 + per_piece // 2)
    for t, n in far[per_piece:2 * per_piece]:
        pass_on(t, n)
    fill_weights(2 + per_piece // 2, n_img)
    take_images(0, 0, img[:, pl.ds(pl.multiple_of(me * part, LANES), part)])
    with jax.named_scope("nearimg"):
        near.wait()
    take_images(1, 0, moved[1])
    for t, n in far[2 * per_piece:]:
        pass_on(t, n)
    for t in range(2, n_img, 2):
        with jax.named_scope(f"post{t}"):
            post_copies[t].wait_recv()
        post_copies[t + 1].start()
    for t, n in far:
        take_rows(t, my_rows[n])

    every_stats[0] = stats[...]
    with jax.named_scope("stat"):
        wait_bytes(every_stats.at[pl.ds(1, n_img * n_proj - 1)], stat_recv)
    evidence = []
    for t in range(n_img):
        every = every_stats[pl.ds(t * n_proj, n_proj)]
        peaks, masses = every[:, 0, :], every[:, 1, :]
        highest = jnp.max(peaks, axis=0, keepdims=True)
        whole = jnp.sum(masses * jnp.exp(peaks - highest), axis=0, keepdims=True)
        evidence.append(highest + jnp.log(whole))
        scale = jnp.exp(peaks[0:1, :] - evidence[t])
        if t % 2:
            with jax.named_scope(f"post{t}"):
                post_copies[t].wait_recv()
        values = every_terms[t].astype(jnp.float32) if t else terms[...].astype(jnp.float32)
        posts_ref[:, t * img_rows:(t + 1) * img_rows] = (values * scale).astype(jnp.bfloat16)

    groups = img_rows // BLOCK
    group = lax.broadcasted_iota(jnp.int32, (1, img_rows), 1) // BLOCK
    placed = jnp.zeros((1, img_rows), jnp.float32)
    for t in range(n_img):
        plan = jnp.zeros((1, img_rows), jnp.int32)
        for g in range(groups):
            plan = jnp.where(group == g, plan_ref[img_from(t) * groups + g], plan)
        for s in range(groups):
            turned, target = evidence[t], plan
            if s:
                turned = pltpu.roll(evidence[t], s * BLOCK, 1)
                target = pltpu.roll(plan, s * BLOCK, 1)
            placed = placed + jnp.where(target == me * groups + group, turned, 0.0)
    ev_ref[...] = placed

    wait_bytes(every_stats.at[pl.ds(1, n_img * n_proj - 1)], stat_send)
    for n, every in enumerate((focus_all, limit_all)):
        wait_bytes(every.at[pl.ds(1, n_img - 1)], small_send.at[n])
    wait_bytes(every_terms.at[pl.ds(1, n_img - 1)], post_send)
    sent, handed = PIECES * PIECE + quarter, PIECES * PIECE + 3 * quarter
    wait_bytes(moved.at[pl.ds(2, n_img - 2), pl.ds(0, sent)], img_send)
    handed_rows = moved.at[pl.ds(2, n_img - 2), pl.ds(0, handed)]
    with jax.named_scope("pass"):
        wait_bytes(handed_rows, pass_recv)
    for t in range(2, n_img):
        for rows in other_rows:
            take_rows(t, rows)
    wait_bytes(handed_rows, pass_send)


def back_kernel(posts_ref, back_img, back_wgt, ev_ref, rec_hbm, placed_hbm, rec, out_sem):
    part = back_img.shape[1]
    step = min(part, 256)
    steps = part // step
    posts = posts_ref[...]
    last = pltpu.make_async_copy(ev_ref, placed_hbm, out_sem.at[steps])
    last.start()
    copies = [last]
    for c in range(steps):
        cols = slice(c * step, (c + 1) * step)
        sums = jnp.dot(posts, back_img[:, cols], preferred_element_type=jnp.float32)
        weights = jnp.dot(posts, back_wgt[:, cols], preferred_element_type=jnp.float32)
        rec[:, cols] = (sums / (weights + 1.0)).astype(jnp.bfloat16)
        copies.append(pltpu.make_async_copy(rec.at[:, cols], rec_hbm.at[:, cols], out_sem.at[c]))
        copies[-1].start()
    for copy in copies:
        copy.wait()


def shards(n_img, n_proj, images, projections, noise_weight, defocus, orient_count, term_limit, block_plan):
    img_rows, width = images.shape
    proj_rows = projections.shape[0]
    part = width // n_img
    x_size = 1 << ((n_proj.bit_length() - 1) // 2)
    vmem = pl.BlockSpec(memory_space=pltpu.VMEM)
    hbm = pl.BlockSpec(memory_space=pl.ANY)
    bf16, f32, i32 = jnp.bfloat16, jnp.float32, jnp.int32
    dma, regular = pltpu.SemaphoreType.DMA, pltpu.SemaphoreType.REGULAR
    held = pl.pallas_call(
        functools.partial(score_kernel, n_img, n_proj, x_size),
        out_shape=(pltpu.VMEM((proj_rows, n_img * img_rows), bf16), pltpu.VMEM((n_img * img_rows, part), bf16),
                   pltpu.VMEM((n_img * img_rows, part), bf16), pltpu.VMEM((1, img_rows), f32)),
        in_specs=[hbm] * 7,
        out_specs=(vmem, vmem, vmem, vmem),
        scratch_shapes=[
            pltpu.VMEM((img_rows, width), bf16),
            pltpu.VMEM((proj_rows, width), bf16),
            pltpu.VMEM((1, width), f32),
            pltpu.VMEM((1, img_rows), f32),
            pltpu.VMEM((1, img_rows), i32),
            pltpu.VMEM((1, img_rows), i32),
            pltpu.SMEM(block_plan.shape, i32),
            pltpu.VMEM((2, img_rows, DEPTH), bf16),
            pltpu.VMEM((2, img_rows, DEPTH), bf16),
            pltpu.VMEM((proj_rows, img_rows), f32),
            pltpu.VMEM((4, img_rows, LANES), f32),
            pltpu.VMEM((n_img, img_rows, part), bf16),
            pltpu.VMEM((n_img * img_rows, part), f32),
            pltpu.VMEM((n_img, 1, img_rows), f32),
            pltpu.VMEM((n_img, 1, img_rows), i32),
            pltpu.VMEM((proj_rows, img_rows), bf16),
            pltpu.VMEM((n_img, proj_rows, img_rows), bf16),
            pltpu.VMEM((2, img_rows), f32),
            pltpu.VMEM((n_img * n_proj, 2, img_rows), f32),
            dma((5,)), dma((width // DEPTH // 2,)), dma((width // DEPTH // 2,)), regular, regular,
            dma((2,)), dma((2,)), dma((2,)), dma, dma((n_img - 2, PIECES + 1)), dma, dma,
            dma, dma((n_img - 1,)), dma, dma,
        ],
        compiler_params=pltpu.CompilerParams(
            collective_id=0, has_side_effects=True, vmem_limit_bytes=54 * 1024 * 1024),
    )(images, projections, noise_weight.reshape(1, -1), defocus.reshape(1, -1), orient_count.reshape(1, -1),
      term_limit.reshape(1, -1), block_plan)
    reconstruction, evidence = pl.pallas_call(
        back_kernel,
        out_shape=(jax.ShapeDtypeStruct((proj_rows, part), bf16), jax.ShapeDtypeStruct((1, img_rows), f32)),
        in_specs=[vmem] * 4,
        out_specs=(hbm, hbm),
        scratch_shapes=[pltpu.VMEM((proj_rows, part), bf16), dma((part // min(part, 256) + 1,))],
        compiler_params=pltpu.CompilerParams(vmem_limit_bytes=16 * 1024 * 1024),
    )(*held)
    return reconstruction, evidence.reshape(-1)


def solution(mesh):
    n_img, n_proj = mesh.shape["img"], mesh.shape["proj"]
    placed = (P("img", None), P("proj", None), P(), P("img"), P("img"), P("img"), P())
    return jax.shard_map(
        functools.partial(shards, n_img, n_proj), mesh=mesh, in_specs=placed,
        out_specs=(P("proj", "img"), P("img")), check_vma=False,
    )
```

```python
import functools
import math

import jax
import jax.numpy as jnp
from jax import lax
from jax.experimental import pallas as pl
from jax.experimental.pallas import tpu as pltpu
from jax.sharding import PartitionSpec as P

BLOCK = 32
PIECES = 2
PIECE = 16
STEP = 256
LANES = 128
DEPTH = 512
MESH = pl.DeviceIdType.MESH
SIN_TERMS = [(-1.0) ** k * math.pi ** (2 * k + 1) / math.factorial(2 * k + 1) for k in range(7)]
COS_TERMS = [(-1.0) ** k * math.pi ** (2 * k) / math.factorial(2 * k) for k in range(8)]


def horner(terms, x):
    total = jnp.full_like(x, terms[-1])
    for term in terms[-2::-1]:
        total = total * x + term
    return total


def sincos_turns(turns):
    rest = turns - jnp.floor(turns + 0.5)
    square = rest * rest
    half_sin = rest * horner(SIN_TERMS, square)
    half_cos = horner(COS_TERMS, square)
    return 2.0 * half_sin * half_cos, 1.0 - 2.0 * half_sin * half_sin


def columns_of(row, rows):
    return jnp.broadcast_to(row, (LANES, rows)).T


def step_sines(row, width):
    sin_d, cos_d = sincos_turns(row * (LANES / width))
    rows = row.shape[1]
    return columns_of(sin_d, rows), columns_of(cos_d, rows)


def sine_start(row, term0, width):
    sin_d, cos_d = step_sines(row, width)
    focus = columns_of(row, row.shape[1])
    sin0, cos0 = sincos_turns(focus * ((term0 + 1.0) / width) + 0.1 / (2.0 * math.pi))
    return sin0, sin0 * cos_d - cos0 * sin_d, 2.0 * cos_d


def wait_bytes(ref, sem):
    pltpu.make_async_copy(ref, ref, sem).wait()


def score_kernel(n_img, n_proj, x_size, img_hbm, proj_hbm, noise_hbm, focus_hbm, count_hbm, limit_hbm, plan_hbm,
                 posts_ref, back_img, back_wgt, near_img, near_wgt, ev_ref,
                 img, proj, noise_ref, focus_ref, count_ref, limit_ref, plan_ref, weighted, weighted_sq, total,
                 sine, moved, contrast, focus_all, limit_all, terms, every_terms, stats, every_stats,
                 load_sem, img_load, proj_load, next_token, all_token,
                 small_send, small_recv, near_sem, img_send, img_recv, pass_send, pass_recv,
                 post_send, post_recv, stat_send, stat_recv):
    me = lax.axis_index("img")
    mine = lax.axis_index("proj")
    img_rows, width = img.shape
    proj_rows = proj.shape[0]
    part = width // n_img
    chips = n_img // 2
    row_y, core = me // 2, lax.rem(me, 2)
    at_x, at_z = lax.rem(mine, x_size), mine // x_size

    def img_to(t):
        return lax.rem(row_y + t // 2, chips) * 2 + lax.rem(core + lax.rem(t, 2), 2)

    def img_from(t):
        return lax.rem(row_y + chips - t // 2, chips) * 2 + lax.rem(core + t % 2, 2)

    odd_x, odd_z = lax.rem(at_x, 2), lax.rem(at_z, 2)
    side = lax.rem(odd_x + odd_z, 2)
    beside_x, beside_z = mine + 1 - 2 * odd_x, mine + x_size * (1 - 2 * odd_z)
    beside_xz = beside_x + beside_z - mine
    quarter = (img_rows - 2 * PIECES * PIECE) // 4

    def half_rows(k, n):
        return pl.ds(pl.multiple_of((k * PIECES + n) * PIECE, PIECE), PIECE)

    def quarter_rows(x, z):
        return pl.ds(pl.multiple_of(2 * PIECES * PIECE + (x * 2 + z) * quarter, 8), quarter)

    def signal(sem, img, proj):
        pl.semaphore_signal(sem, inc=1, device_id={"img": img, "proj": proj}, device_id_type=MESH)

    barrier = pltpu.get_barrier_semaphore()
    partner, first_core = img_to(1), core == 0

    def greet_next(t, proj):
        signal(barrier, img_to(t) - lax.rem(img_to(t), 2), proj)

    for t in range(2, n_img, 2):
        greet_next(t, mine)
    pl.when(jnp.logical_not(first_core))(lambda: signal(barrier, partner, mine))

    def greet_all(proj, carry):
        for chip in range(chips):
            pl.when(jnp.logical_or(chip * 2 + 1 != me, proj != mine))(lambda: signal(barrier, chip * 2 + 1, proj))
        return carry

    def meet_all():
        with jax.named_scope("all"):
            @pl.when(jnp.logical_not(first_core))
            def _():
                pl.semaphore_wait(barrier, n_img * n_proj - 1)
                signal(all_token, partner, mine)
            pl.when(first_core)(lambda: pl.semaphore_wait(all_token, 1))

    small_loads = [pltpu.make_async_copy(source, target, load_sem.at[n]) for n, (source, target) in enumerate(
        ((focus_hbm, focus_ref), (limit_hbm, limit_ref), (noise_hbm, noise_ref), (count_hbm, count_ref),
         (plan_hbm, plan_ref)))]
    wide = 2 * DEPTH
    steps = width // wide

    def load_img(n):
        cols = pl.ds(pl.multiple_of(n * wide, wide), wide)
        return pltpu.make_async_copy(img_hbm.at[:, cols], img.at[:, cols], img_load.at[n])

    def load_proj(n):
        cols = pl.ds(pl.multiple_of(n * wide, wide), wide)
        return pltpu.make_async_copy(proj_hbm.at[:, cols], proj.at[:, cols], proj_load.at[n])

    for load in small_loads[:3]:
        load.start()
    load_img(0).start()
    for n in range(steps):
        load_proj(n).start()
        if n + 1 < steps:
            load_img(n + 1).start()
    for load in small_loads[3:]:
        load.start()
    with jax.named_scope('greet'):
        lax.fori_loop(0, n_proj, greet_all, 0)
    my_rows = [quarter_rows(odd_x, odd_z)] + [half_rows(side, n) for n in range(PIECES)]

    def move_img(t, n):
        slab = pl.ds(pl.multiple_of(img_to(t) * part, LANES), part)
        return pltpu.make_async_remote_copy(
            src_ref=img_hbm.at[my_rows[n], slab], dst_ref=moved.at[t, my_rows[n], :], send_sem=img_send,
            recv_sem=img_recv.at[t - 2, n], device_id={"img": img_to(t)}, device_id_type=MESH)

    def pass_rows(t, rows, proj, sem):
        held = moved.at[t, rows, :]
        pltpu.make_async_remote_copy(
            src_ref=held, dst_ref=held, send_sem=pass_send, recv_sem=sem, device_id={"proj": proj},
            device_id_type=MESH).start()

    near = pltpu.make_async_remote_copy(
        src_ref=img_hbm.at[:, pl.ds(pl.multiple_of(img_to(1) * part, LANES), part)], dst_ref=moved.at[1],
        send_sem=near_sem.at[0], recv_sem=near_sem.at[1], device_id={"img": img_to(1)}, device_id_type=MESH)
    small = [pltpu.make_async_remote_copy(
        src_ref=ref, dst_ref=dst.at[t], send_sem=small_send.at[n], recv_sem=small_recv.at[n],
        device_id={"img": img_to(t)}, device_id_type=MESH)
        for t in range(1, n_img) for n, (ref, dst) in enumerate(((focus_hbm, focus_all), (limit_hbm, limit_all)))]
    far = [(t, n) for n in range(PIECES + 1) for t in range(2, n_img)]

    def send_images():
        for copy in small:
            copy.start()
        for t, n in far:
            move_img(t, n).start()
        near.start()

    @pl.when(first_core)
    def _():
        with jax.named_scope("near"):
            pl.semaphore_wait(barrier, 2 * (chips - 1) + 1)
        signal(next_token, partner, mine)
        send_images()

    with jax.named_scope("small"):
        small_loads[0].wait()
        small_loads[1].wait()

    lane = lax.broadcasted_iota(jnp.int32, (1, LANES), 1).astype(jnp.float32)
    sine[0], sine[1], sine[2] = sine_start(focus_ref[...], lane, width)
    sine[3] = columns_of(limit_ref[...].astype(jnp.float32), img_rows)
    total[...] = jnp.zeros_like(total)
    small_loads[2].wait()
    contract = (((1,), (1,)), ((), ()))
    strip = 16

    def terms_chunk(c, slot):
        starts = [pl.multiple_of(c * DEPTH + k * LANES, LANES) for k in range(DEPTH // LANES)]
        noise = [noise_ref[:, pl.ds(start, LANES)] for start in starts]
        term = [lane + start.astype(jnp.float32) for start in starts]
        for r in range(img_rows // strip):
            rows = slice(r * strip, (r + 1) * strip)
            sin_v, sin_before, turn, limit = sine[0, rows], sine[1, rows], sine[2, rows], sine[3, rows]
            for k, start in enumerate(starts):
                cols = slice(k * LANES, (k + 1) * LANES)
                noisy = jnp.where(term[k] < limit, sin_v, 0.0) * noise[k]
                pixels = img[rows, pl.ds(start, LANES)].astype(jnp.float32)
                weighted[slot, rows, cols] = (noisy * pixels).astype(jnp.bfloat16)
                weighted_sq[slot, rows, cols] = (noisy * (-0.5 * sin_v)).astype(jnp.bfloat16)
                sin_v, sin_before = turn * sin_v - sin_before, sin_v
            sine[0, rows] = sin_v
            sine[1, rows] = sin_before

    def score_chunk(c, slot):
        rows = proj[:, pl.ds(pl.multiple_of(c * DEPTH, DEPTH), DEPTH)]
        got = lax.dot_general(rows, weighted[slot], contract, preferred_element_type=jnp.float32)
        got = got + lax.dot_general(rows * rows, weighted_sq[slot], contract, preferred_element_type=jnp.float32)
        total[...] += got

    with jax.named_scope("img0"):
        load_img(0).wait()
    terms_chunk(jnp.int32(0), 0)

    def score_step(i, carry):
        with jax.named_scope("loads"):
            load_proj(i).wait()
            pl.when(i + 1 < steps)(lambda: load_img(i + 1).wait())

        @pl.when(jnp.logical_and(i == 0, jnp.logical_not(first_core)))
        def _():
            with jax.named_scope("near"):
                pl.semaphore_wait(next_token, 1)
            send_images()

        score_chunk(2 * i, 0)
        terms_chunk(2 * i + 1, 1)
        score_chunk(2 * i + 1, 1)
        terms_chunk(jnp.minimum(2 * i + 2, width // DEPTH - 1), 0)
        return carry

    lax.fori_loop(0, steps, score_step, 0)

    with jax.named_scope("smax"):
        small_loads[3].wait()
        small_loads[4].wait()
    scores = total[...]
    orient = lax.broadcasted_iota(jnp.int32, (proj_rows, img_rows), 0) + mine * proj_rows
    significant = orient < count_ref[...]
    masked = jnp.where(significant, scores, -1e30)
    peak = jnp.max(masked, axis=0, keepdims=True)
    expo = jnp.where(significant, jnp.exp(masked - peak), 0.0)
    stats[0:1, :] = peak
    stats[1:2, :] = jnp.sum(expo, axis=0, keepdims=True)
    terms[...] = expo.astype(jnp.bfloat16)

    rows_of = [img_to(t) for t in range(n_img)]

    def send_stats(target, carry):
        ahead = target - mine
        ahead = jnp.where(ahead < 0, ahead + n_proj, ahead)
        for t in range(n_img):
            copy = pltpu.make_async_remote_copy(
                src_ref=stats, dst_ref=every_stats.at[t * n_proj + ahead], send_sem=stat_send, recv_sem=stat_recv,
                device_id={"img": rows_of[t], "proj": target}, device_id_type=MESH)
            if t:
                copy.start()
            else:
                pl.when(target != mine)(copy.start)
        return carry

    def pass_on(t, n):
        with jax.named_scope(f"mv{t}{n}"):
            move_img(t, n).wait_recv()
        if n:
            pass_rows(t, my_rows[n], (beside_x, beside_z)[(n + t) % 2], pass_recv.at[1])
        else:
            for proj in (beside_xz, beside_x, beside_z):
                pass_rows(t, my_rows[0], proj, pass_recv.at[0])

    meet_all()
    with jax.named_scope("send"):
        lax.fori_loop(0, n_proj, send_stats, 0)

    post_copies = {t: pltpu.make_async_remote_copy(
        src_ref=terms, dst_ref=every_terms.at[t], send_sem=post_send, recv_sem=post_recv.at[t - 1],
        device_id={"img": img_to(t)}, device_id_type=MESH) for t in (1, *range(2, n_img, 2))}
    for t in range(2, n_img, 2):
        post_copies[t + 1] = pltpu.make_async_remote_copy(
            src_ref=every_terms.at[t], dst_ref=every_terms.at[t + 1], send_sem=post_send,
            recv_sem=post_recv.at[t], device_id={"img": img_to(1)}, device_id_type=MESH)
    post_copies[1].start()

    per_piece = n_img - 2
    for t, n in far[:per_piece]:
        pass_on(t, n)
    for t in range(2, n_img, 2):
        post_copies[t].start()

    term0 = lane + (me * part).astype(jnp.float32)

    def weights_block(t, carry):
        sine[0], sine[1], sine[2] = sine_start(focus_all[t], term0, width)
        sine[3] = columns_of(limit_all[t].astype(jnp.float32), img_rows)
        for r in range(img_rows // strip):
            inside = slice(r * strip, (r + 1) * strip)
            rows = pl.ds(pl.multiple_of(t * img_rows + r * strip, strip), strip)
            sin_v, sin_before, turn, limit = sine[0, inside], sine[1, inside], sine[2, inside], sine[3, inside]
            for c in range(part // LANES):
                cols = slice(c * LANES, (c + 1) * LANES)
                kept = jnp.where(term0 + float(c * LANES) < limit, sin_v, 0.0)
                contrast[rows, cols] = kept
                back_wgt[rows, cols] = (kept * sin_v).astype(jnp.bfloat16)
                sin_v, sin_before = turn * sin_v - sin_before, sin_v
        return carry

    def take_images(t, first, pixels):
        rows = pl.ds(pl.multiple_of(t * img_rows + first, 8), pixels.shape[0])
        back_img[rows, :] = (contrast[rows, :] * pixels.astype(jnp.float32)).astype(jnp.bfloat16)

    def take_rows(t, rows):
        take_images(t, rows.start, moved[t, rows, :])

    quarter_others = [quarter_rows(1 - odd_x, odd_z), quarter_rows(odd_x, 1 - odd_z), quarter_rows(1 - odd_x, 1 - odd_z)]
    half_others = [half_rows(1 - side, n) for n in range(PIECES)]

    focus_all[0] = focus_ref[...]
    limit_all[0] = limit_ref[...]
    fill_weights = lambda lo, hi: lax.fori_loop(lo, hi, weights_block, 0)
    fill_weights(0, 1)
    with jax.named_scope("smallx"):
        for n, every in enumerate((focus_all, limit_all)):
            wait_bytes(every.at[pl.ds(1, n_img - 1)], small_recv.at[n])
    fill_weights(1, 2)
    fill_weights(2, 2 + per_piece // 2)
    for t, n in far[per_piece:2 * per_piece]:
        pass_on(t, n)
    fill_weights(2 + per_piece // 2, n_img)
    take_images(0, 0, img[:, pl.ds(pl.multiple_of(me * part, LANES), part)])
    with jax.named_scope("nearimg"):
        near.wait()
    take_images(1, 0, moved[1])
    for t, n in far[2 * per_piece:]:
        pass_on(t, n)
    for t in range(2, n_img, 2):
        with jax.named_scope(f"post{t}"):
            post_copies[t].wait_recv()
        post_copies[t + 1].start()
    for t, n in far:
        take_rows(t, my_rows[n])

    every_stats[0] = stats[...]
    with jax.named_scope("stat"):
        wait_bytes(every_stats.at[pl.ds(1, n_img * n_proj - 1)], stat_recv)
    evidence, scales = [], []
    for t in range(n_img):
        every = every_stats[pl.ds(t * n_proj, n_proj)]
        peaks, masses = every[:, 0, :], every[:, 1, :]
        highest = jnp.max(peaks, axis=0, keepdims=True)
        whole = jnp.sum(masses * jnp.exp(peaks - highest), axis=0, keepdims=True)
        evidence.append(highest + jnp.log(whole))
        scale = jnp.exp(peaks[0:1, :] - evidence[t])
        scales.append(scale)

    def place_posts(t):
        if t % 2:
            with jax.named_scope(f"post{t}"):
                post_copies[t].wait_recv()
        values = every_terms[t].astype(jnp.float32) if t else terms[...].astype(jnp.float32)
        posts_ref[:, t * img_rows:(t + 1) * img_rows] = (values * scales[t]).astype(jnp.bfloat16)

    for t in range(2):
        place_posts(t)
    near_cols = 2 * img_rows
    for c in range(part // STEP):
        cols = slice(c * STEP, (c + 1) * STEP)
        near_img[:, cols] = jnp.dot(posts_ref[:, :near_cols], back_img[:near_cols, cols],
                                    preferred_element_type=jnp.float32)
        near_wgt[:, cols] = jnp.dot(posts_ref[:, :near_cols], back_wgt[:near_cols, cols],
                                    preferred_element_type=jnp.float32)

    for t in range(2, n_img):
        place_posts(t)

    groups = img_rows // BLOCK
    group = lax.broadcasted_iota(jnp.int32, (1, img_rows), 1) // BLOCK
    placed = jnp.zeros((1, img_rows), jnp.float32)
    for t in range(n_img):
        plan = jnp.zeros((1, img_rows), jnp.int32)
        for g in range(groups):
            plan = jnp.where(group == g, plan_ref[img_from(t) * groups + g], plan)
        for s in range(groups):
            turned, target = evidence[t], plan
            if s:
                turned = pltpu.roll(evidence[t], s * BLOCK, 1)
                target = pltpu.roll(plan, s * BLOCK, 1)
            placed = placed + jnp.where(target == me * groups + group, turned, 0.0)
    ev_ref[...] = placed

    wait_bytes(every_stats.at[pl.ds(1, n_img * n_proj - 1)], stat_send)
    for n, every in enumerate((focus_all, limit_all)):
        wait_bytes(every.at[pl.ds(1, n_img - 1)], small_send.at[n])
    wait_bytes(every_terms.at[pl.ds(1, n_img - 1)], post_send)
    def far_bytes(rows):
        return moved.at[pl.ds(2, n_img - 2), pl.ds(0, rows)]

    wait_bytes(far_bytes(PIECES * PIECE + quarter), img_send)
    with jax.named_scope("quart"):
        wait_bytes(moved.at[pl.ds(2, n_img - 2), pl.ds(0, 3 * quarter)], pass_recv.at[0])
    for t in range(2, n_img):
        for rows in quarter_others:
            take_rows(t, rows)
    with jax.named_scope("half"):
        wait_bytes(far_bytes(PIECES * PIECE), pass_recv.at[1])
    for t in range(2, n_img):
        for rows in half_others:
            take_rows(t, rows)
    wait_bytes(far_bytes(PIECES * PIECE + 3 * quarter), pass_send)


def back_kernel(near_cols, posts_ref, back_img, back_wgt, near_img, near_wgt, ev_ref, rec_hbm, placed_hbm, rec, out_sem):
    part = back_img.shape[1]
    steps = part // STEP
    posts = posts_ref[:, near_cols:]
    last = pltpu.make_async_copy(ev_ref, placed_hbm, out_sem.at[steps])
    last.start()
    copies = [last]
    for c in range(steps):
        cols = slice(c * STEP, (c + 1) * STEP)
        sums = near_img[:, cols] + jnp.dot(posts, back_img[near_cols:, cols], preferred_element_type=jnp.float32)
        weights = near_wgt[:, cols] + jnp.dot(posts, back_wgt[near_cols:, cols], preferred_element_type=jnp.float32)
        rec[:, cols] = (sums / (weights + 1.0)).astype(jnp.bfloat16)
        copies.append(pltpu.make_async_copy(rec.at[:, cols], rec_hbm.at[:, cols], out_sem.at[c]))
        copies[-1].start()
    for copy in copies:
        copy.wait()


def shards(n_img, n_proj, images, projections, noise_weight, defocus, orient_count, term_limit, block_plan):
    img_rows, width = images.shape
    proj_rows = projections.shape[0]
    part = width // n_img
    x_size = 1 << ((n_proj.bit_length() - 1) // 2)
    vmem = pl.BlockSpec(memory_space=pltpu.VMEM)
    hbm = pl.BlockSpec(memory_space=pl.ANY)
    bf16, f32, i32 = jnp.bfloat16, jnp.float32, jnp.int32
    dma, regular = pltpu.SemaphoreType.DMA, pltpu.SemaphoreType.REGULAR
    held = pl.pallas_call(
        functools.partial(score_kernel, n_img, n_proj, x_size),
        out_shape=(pltpu.VMEM((proj_rows, n_img * img_rows), bf16), pltpu.VMEM((n_img * img_rows, part), bf16),
                   pltpu.VMEM((n_img * img_rows, part), bf16), pltpu.VMEM((proj_rows, part), f32),
                   pltpu.VMEM((proj_rows, part), f32), pltpu.VMEM((1, img_rows), f32)),
        in_specs=[hbm] * 7,
        out_specs=(vmem,) * 6,
        scratch_shapes=[
            pltpu.VMEM((img_rows, width), bf16),
            pltpu.VMEM((proj_rows, width), bf16),
            pltpu.VMEM((1, width), f32),
            pltpu.VMEM((1, img_rows), f32),
            pltpu.VMEM((1, img_rows), i32),
            pltpu.VMEM((1, img_rows), i32),
            pltpu.SMEM(block_plan.shape, i32),
            pltpu.VMEM((2, img_rows, DEPTH), bf16),
            pltpu.VMEM((2, img_rows, DEPTH), bf16),
            pltpu.VMEM((proj_rows, img_rows), f32),
            pltpu.VMEM((4, img_rows, LANES), f32),
            pltpu.VMEM((n_img, img_rows, part), bf16),
            pltpu.VMEM((n_img * img_rows, part), f32),
            pltpu.VMEM((n_img, 1, img_rows), f32),
            pltpu.VMEM((n_img, 1, img_rows), i32),
            pltpu.VMEM((proj_rows, img_rows), bf16),
            pltpu.VMEM((n_img, proj_rows, img_rows), bf16),
            pltpu.VMEM((2, img_rows), f32),
            pltpu.VMEM((n_img * n_proj, 2, img_rows), f32),
            dma((5,)), dma((width // DEPTH // 2,)), dma((width // DEPTH // 2,)), regular, regular,
            dma((2,)), dma((2,)), dma((2,)), dma, dma((n_img - 2, PIECES + 1)), dma, dma((2,)),
            dma, dma((n_img - 1,)), dma, dma,
        ],
        compiler_params=pltpu.CompilerParams(
            collective_id=0, has_side_effects=True, vmem_limit_bytes=54 * 1024 * 1024),
    )(images, projections, noise_weight.reshape(1, -1), defocus.reshape(1, -1), orient_count.reshape(1, -1),
      term_limit.reshape(1, -1), block_plan)
    reconstruction, evidence = pl.pallas_call(
        functools.partial(back_kernel, 2 * img_rows),
        out_shape=(jax.ShapeDtypeStruct((proj_rows, part), bf16), jax.ShapeDtypeStruct((1, img_rows), f32)),
        in_specs=[vmem] * 6,
        out_specs=(hbm, hbm),
        scratch_shapes=[pltpu.VMEM((proj_rows, part), bf16), dma((part // STEP + 1,))],
        compiler_params=pltpu.CompilerParams(vmem_limit_bytes=16 * 1024 * 1024),
    )(*held)
    return reconstruction, evidence.reshape(-1)


def solution(mesh):
    n_img, n_proj = mesh.shape["img"], mesh.shape["proj"]
    placed = (P("img", None), P("proj", None), P(), P("img"), P("img"), P("img"), P())
    return jax.shard_map(
        functools.partial(shards, n_img, n_proj), mesh=mesh, in_specs=placed,
        out_specs=(P("proj", "img"), P("img")), check_vma=False,
    )
```

```python
import functools
import math

import jax
import jax.numpy as jnp
from jax import lax
from jax.experimental import pallas as pl
from jax.experimental.pallas import tpu as pltpu
from jax.sharding import PartitionSpec as P

BLOCK = 32
PIECES = 1
PIECE = 16
DIRECT = 32
STEP = 256
LANES = 128
DEPTH = 512
MESH = pl.DeviceIdType.MESH
SIN_TERMS = [(-1.0) ** k * math.pi ** (2 * k + 1) / math.factorial(2 * k + 1) for k in range(7)]
COS_TERMS = [(-1.0) ** k * math.pi ** (2 * k) / math.factorial(2 * k) for k in range(8)]


def horner(terms, x):
    total = jnp.full_like(x, terms[-1])
    for term in terms[-2::-1]:
        total = total * x + term
    return total


def sincos_turns(turns):
    rest = turns - jnp.floor(turns + 0.5)
    square = rest * rest
    half_sin = rest * horner(SIN_TERMS, square)
    half_cos = horner(COS_TERMS, square)
    return 2.0 * half_sin * half_cos, 1.0 - 2.0 * half_sin * half_sin


def columns_of(row, rows):
    return jnp.broadcast_to(row, (LANES, rows)).T


def step_sines(row, width):
    sin_d, cos_d = sincos_turns(row * (LANES / width))
    rows = row.shape[1]
    return columns_of(sin_d, rows), columns_of(cos_d, rows)


def sine_start(row, term0, width):
    sin_d, cos_d = step_sines(row, width)
    focus = columns_of(row, row.shape[1])
    sin0, cos0 = sincos_turns(focus * ((term0 + 1.0) / width) + 0.1 / (2.0 * math.pi))
    return sin0, sin0 * cos_d - cos0 * sin_d, 2.0 * cos_d


def wait_bytes(ref, sem):
    pltpu.make_async_copy(ref, ref, sem).wait()


def score_kernel(n_img, n_proj, x_size, img_hbm, proj_hbm, noise_hbm, focus_hbm, count_hbm, limit_hbm, plan_hbm,
                 posts_ref, back_img, back_wgt, near_img, near_wgt, ev_ref,
                 img, proj, noise_ref, focus_ref, count_ref, limit_ref, plan_ref, weighted, weighted_sq, total,
                 sine, moved, contrast, focus_all, limit_all, terms, every_terms, stats, every_stats,
                 load_sem, img_load, proj_load, next_token, all_token,
                 small_send, small_recv, near_sem, img_send, img_recv, pass_send, pass_recv,
                 post_send, post_recv, stat_send, stat_recv):
    me = lax.axis_index("img")
    mine = lax.axis_index("proj")
    img_rows, width = img.shape
    proj_rows = proj.shape[0]
    part = width // n_img
    chips = n_img // 2
    row_y, core = me // 2, lax.rem(me, 2)
    at_x, at_z = lax.rem(mine, x_size), mine // x_size

    def img_to(t):
        return lax.rem(row_y + t // 2, chips) * 2 + lax.rem(core + lax.rem(t, 2), 2)

    def img_from(t):
        return lax.rem(row_y + chips - t // 2, chips) * 2 + lax.rem(core + t % 2, 2)

    odd_x, odd_z = lax.rem(at_x, 2), lax.rem(at_z, 2)
    side = lax.rem(odd_x + odd_z, 2)
    beside_x, beside_z = mine + 1 - 2 * odd_x, mine + x_size * (1 - 2 * odd_z)
    beside_xz = beside_x + beside_z - mine
    quarter = (img_rows - 2 * PIECES * PIECE - DIRECT) // 4

    def half_rows(k, n):
        return pl.ds(pl.multiple_of((k * PIECES + n) * PIECE, PIECE), PIECE)

    def quarter_rows(x, z):
        return pl.ds(pl.multiple_of(2 * PIECES * PIECE + (x * 2 + z) * quarter, 8), quarter)

    def signal(sem, img, proj):
        pl.semaphore_signal(sem, inc=1, device_id={"img": img, "proj": proj}, device_id_type=MESH)

    barrier = pltpu.get_barrier_semaphore()
    partner, first_core = img_to(1), core == 0

    def greet_next(t, proj):
        signal(barrier, img_to(t) - lax.rem(img_to(t), 2), proj)

    for t in range(2, n_img, 2):
        greet_next(t, mine)
    pl.when(jnp.logical_not(first_core))(lambda: signal(barrier, partner, mine))

    def greet_all(proj, carry):
        for chip in range(chips):
            pl.when(jnp.logical_or(chip * 2 + 1 != me, proj != mine))(lambda: signal(barrier, chip * 2 + 1, proj))
        return carry

    def meet_all():
        with jax.named_scope("all"):
            @pl.when(jnp.logical_not(first_core))
            def _():
                pl.semaphore_wait(barrier, n_img * n_proj - 1)
                signal(all_token, partner, mine)
            pl.when(first_core)(lambda: pl.semaphore_wait(all_token, 1))

    small_loads = [pltpu.make_async_copy(source, target, load_sem.at[n]) for n, (source, target) in enumerate(
        ((focus_hbm, focus_ref), (limit_hbm, limit_ref), (noise_hbm, noise_ref), (count_hbm, count_ref),
         (plan_hbm, plan_ref)))]
    wide = 2 * DEPTH
    steps = width // wide

    def load_img(n):
        cols = pl.ds(pl.multiple_of(n * wide, wide), wide)
        return pltpu.make_async_copy(img_hbm.at[:, cols], img.at[:, cols], img_load.at[n])

    def load_proj(n):
        cols = pl.ds(pl.multiple_of(n * wide, wide), wide)
        return pltpu.make_async_copy(proj_hbm.at[:, cols], proj.at[:, cols], proj_load.at[n])

    for load in small_loads[:3]:
        load.start()
    load_img(0).start()
    for n in range(steps):
        load_proj(n).start()
        if n + 1 < steps:
            load_img(n + 1).start()
    for load in small_loads[3:]:
        load.start()
    with jax.named_scope('greet'):
        lax.fori_loop(0, n_proj, greet_all, 0)
    my_rows = [quarter_rows(odd_x, odd_z)] + [half_rows(side, n) for n in range(PIECES)]
    my_rows.append(pl.ds(img_rows - DIRECT, DIRECT))

    def move_img(t, n):
        slab = pl.ds(pl.multiple_of(img_to(t) * part, LANES), part)
        return pltpu.make_async_remote_copy(
            src_ref=img_hbm.at[my_rows[n], slab], dst_ref=moved.at[t, my_rows[n], :], send_sem=img_send,
            recv_sem=img_recv.at[t - 2, n], device_id={"img": img_to(t)}, device_id_type=MESH)

    def pass_rows(t, rows, proj, sem):
        held = moved.at[t, rows, :]
        pltpu.make_async_remote_copy(
            src_ref=held, dst_ref=held, send_sem=pass_send, recv_sem=sem, device_id={"proj": proj},
            device_id_type=MESH).start()

    near = pltpu.make_async_remote_copy(
        src_ref=img_hbm.at[:, pl.ds(pl.multiple_of(img_to(1) * part, LANES), part)], dst_ref=moved.at[1],
        send_sem=near_sem.at[0], recv_sem=near_sem.at[1], device_id={"img": img_to(1)}, device_id_type=MESH)
    small = [pltpu.make_async_remote_copy(
        src_ref=ref, dst_ref=dst.at[t], send_sem=small_send.at[n], recv_sem=small_recv.at[n],
        device_id={"img": img_to(t)}, device_id_type=MESH)
        for t in range(1, n_img) for n, (ref, dst) in enumerate(((focus_hbm, focus_all), (limit_hbm, limit_all)))]
    far = [(t, n) for n in range(PIECES + 1) for t in range(2, n_img)]

    def send_images():
        for copy in small:
            copy.start()
        for t, n in far:
            move_img(t, n).start()
        near.start()
        for t in range(2, n_img, 2):
            move_img(t, PIECES + 1).start()

    @pl.when(first_core)
    def _():
        with jax.named_scope("near"):
            pl.semaphore_wait(barrier, 2 * (chips - 1) + 1)
        signal(next_token, partner, mine)
        send_images()

    with jax.named_scope("small"):
        small_loads[0].wait()
        small_loads[1].wait()

    lane = lax.broadcasted_iota(jnp.int32, (1, LANES), 1).astype(jnp.float32)
    sine[0], sine[1], sine[2] = sine_start(focus_ref[...], lane, width)
    sine[3] = columns_of(limit_ref[...].astype(jnp.float32), img_rows)
    total[...] = jnp.zeros_like(total)
    small_loads[2].wait()
    contract = (((1,), (1,)), ((), ()))
    strip = 16

    def terms_chunk(c, slot):
        starts = [pl.multiple_of(c * DEPTH + k * LANES, LANES) for k in range(DEPTH // LANES)]
        noise = [noise_ref[:, pl.ds(start, LANES)] for start in starts]
        term = [lane + start.astype(jnp.float32) for start in starts]
        for r in range(img_rows // strip):
            rows = slice(r * strip, (r + 1) * strip)
            sin_v, sin_before, turn, limit = sine[0, rows], sine[1, rows], sine[2, rows], sine[3, rows]
            for k, start in enumerate(starts):
                cols = slice(k * LANES, (k + 1) * LANES)
                noisy = jnp.where(term[k] < limit, sin_v, 0.0) * noise[k]
                pixels = img[rows, pl.ds(start, LANES)].astype(jnp.float32)
                weighted[slot, rows, cols] = (noisy * pixels).astype(jnp.bfloat16)
                weighted_sq[slot, rows, cols] = (noisy * (-0.5 * sin_v)).astype(jnp.bfloat16)
                sin_v, sin_before = turn * sin_v - sin_before, sin_v
            sine[0, rows] = sin_v
            sine[1, rows] = sin_before

    def score_chunk(c, slot):
        rows = proj[:, pl.ds(pl.multiple_of(c * DEPTH, DEPTH), DEPTH)]
        got = lax.dot_general(rows, weighted[slot], contract, preferred_element_type=jnp.float32)
        got = got + lax.dot_general(rows * rows, weighted_sq[slot], contract, preferred_element_type=jnp.float32)
        total[...] += got

    with jax.named_scope("img0"):
        load_img(0).wait()
    terms_chunk(jnp.int32(0), 0)

    def score_step(i, carry):
        with jax.named_scope("loads"):
            load_proj(i).wait()
            pl.when(i + 1 < steps)(lambda: load_img(i + 1).wait())

        @pl.when(jnp.logical_and(i == 0, jnp.logical_not(first_core)))
        def _():
            with jax.named_scope("near"):
                pl.semaphore_wait(next_token, 1)
            send_images()

        score_chunk(2 * i, 0)
        terms_chunk(2 * i + 1, 1)
        score_chunk(2 * i + 1, 1)
        terms_chunk(jnp.minimum(2 * i + 2, width // DEPTH - 1), 0)
        return carry

    lax.fori_loop(0, steps, score_step, 0)

    with jax.named_scope("smax"):
        small_loads[3].wait()
        small_loads[4].wait()
    scores = total[...]
    orient = lax.broadcasted_iota(jnp.int32, (proj_rows, img_rows), 0) + mine * proj_rows
    significant = orient < count_ref[...]
    masked = jnp.where(significant, scores, -1e30)
    peak = jnp.max(masked, axis=0, keepdims=True)
    expo = jnp.where(significant, jnp.exp(masked - peak), 0.0)
    stats[0:1, :] = peak
    stats[1:2, :] = jnp.sum(expo, axis=0, keepdims=True)
    terms[...] = expo.astype(jnp.bfloat16)

    rows_of = [img_to(t) for t in range(n_img)]

    def send_stats(target, carry):
        ahead = target - mine
        ahead = jnp.where(ahead < 0, ahead + n_proj, ahead)
        for t in range(n_img):
            copy = pltpu.make_async_remote_copy(
                src_ref=stats, dst_ref=every_stats.at[t * n_proj + ahead], send_sem=stat_send, recv_sem=stat_recv,
                device_id={"img": rows_of[t], "proj": target}, device_id_type=MESH)
            if t:
                copy.start()
            else:
                pl.when(target != mine)(copy.start)
        return carry

    def pass_on(t, n):
        with jax.named_scope(f"mv{t}{n}"):
            move_img(t, n).wait_recv()
        if n:
            pass_rows(t, my_rows[n], (beside_x, beside_z)[(n + t) % 2], pass_recv.at[1])
        else:
            for proj in (beside_xz, beside_x, beside_z):
                pass_rows(t, my_rows[0], proj, pass_recv.at[0])

    meet_all()
    with jax.named_scope("send"):
        lax.fori_loop(0, n_proj, send_stats, 0)

    post_copies = {t: pltpu.make_async_remote_copy(
        src_ref=terms, dst_ref=every_terms.at[t], send_sem=post_send, recv_sem=post_recv.at[t - 1],
        device_id={"img": img_to(t)}, device_id_type=MESH) for t in (1, *range(2, n_img, 2))}
    for t in range(2, n_img, 2):
        post_copies[t + 1] = pltpu.make_async_remote_copy(
            src_ref=every_terms.at[t], dst_ref=every_terms.at[t + 1], send_sem=post_send,
            recv_sem=post_recv.at[t], device_id={"img": img_to(1)}, device_id_type=MESH)
    post_copies[1].start()

    per_piece = n_img - 2
    for t, n in far[:per_piece]:
        pass_on(t, n)
    for t in range(2, n_img, 2):
        post_copies[t].start()
    for t in range(3, n_img, 2):
        move_img(t, PIECES + 1).start()

    term0 = lane + (me * part).astype(jnp.float32)

    def weights_block(t, carry):
        sine[0], sine[1], sine[2] = sine_start(focus_all[t], term0, width)
        sine[3] = columns_of(limit_all[t].astype(jnp.float32), img_rows)
        for r in range(img_rows // strip):
            inside = slice(r * strip, (r + 1) * strip)
            rows = pl.ds(pl.multiple_of(t * img_rows + r * strip, strip), strip)
            sin_v, sin_before, turn, limit = sine[0, inside], sine[1, inside], sine[2, inside], sine[3, inside]
            for c in range(part // LANES):
                cols = slice(c * LANES, (c + 1) * LANES)
                kept = jnp.where(term0 + float(c * LANES) < limit, sin_v, 0.0)
                contrast[rows, cols] = kept
                back_wgt[rows, cols] = (kept * sin_v).astype(jnp.bfloat16)
                sin_v, sin_before = turn * sin_v - sin_before, sin_v
        return carry

    def take_images(t, first, pixels):
        rows = pl.ds(pl.multiple_of(t * img_rows + first, 8), pixels.shape[0])
        back_img[rows, :] = (contrast[rows, :] * pixels.astype(jnp.float32)).astype(jnp.bfloat16)

    def take_rows(t, rows):
        take_images(t, rows.start, moved[t, rows, :])

    quarter_others = [quarter_rows(1 - odd_x, odd_z), quarter_rows(odd_x, 1 - odd_z), quarter_rows(1 - odd_x, 1 - odd_z)]
    half_others = [half_rows(1 - side, n) for n in range(PIECES)]

    focus_all[0] = focus_ref[...]
    limit_all[0] = limit_ref[...]
    fill_weights = lambda lo, hi: lax.fori_loop(lo, hi, weights_block, 0)
    fill_weights(0, 1)
    with jax.named_scope("smallx"):
        for n, every in enumerate((focus_all, limit_all)):
            wait_bytes(every.at[pl.ds(1, n_img - 1)], small_recv.at[n])
    fill_weights(1, 2)
    fill_weights(2, 2 + per_piece // 2)
    for t, n in far[per_piece:2 * per_piece]:
        pass_on(t, n)
    fill_weights(2 + per_piece // 2, n_img)
    take_images(0, 0, img[:, pl.ds(pl.multiple_of(me * part, LANES), part)])
    with jax.named_scope("nearimg"):
        near.wait()
    take_images(1, 0, moved[1])
    for t, n in far[2 * per_piece:]:
        pass_on(t, n)
    for t in range(2, n_img, 2):
        with jax.named_scope(f"post{t}"):
            post_copies[t].wait_recv()
        post_copies[t + 1].start()
    for t, n in far:
        take_rows(t, my_rows[n])

    every_stats[0] = stats[...]
    with jax.named_scope("stat"):
        wait_bytes(every_stats.at[pl.ds(1, n_img * n_proj - 1)], stat_recv)
    evidence, scales = [], []
    for t in range(n_img):
        every = every_stats[pl.ds(t * n_proj, n_proj)]
        peaks, masses = every[:, 0, :], every[:, 1, :]
        highest = jnp.max(peaks, axis=0, keepdims=True)
        whole = jnp.sum(masses * jnp.exp(peaks - highest), axis=0, keepdims=True)
        evidence.append(highest + jnp.log(whole))
        scale = jnp.exp(peaks[0:1, :] - evidence[t])
        scales.append(scale)

    def place_posts(t):
        if t % 2:
            with jax.named_scope(f"post{t}"):
                post_copies[t].wait_recv()
        values = every_terms[t].astype(jnp.float32) if t else terms[...].astype(jnp.float32)
        posts_ref[:, t * img_rows:(t + 1) * img_rows] = (values * scales[t]).astype(jnp.bfloat16)

    for t in range(2):
        place_posts(t)
    near_cols = 2 * img_rows
    for c in range(part // STEP):
        cols = slice(c * STEP, (c + 1) * STEP)
        near_img[:, cols] = jnp.dot(posts_ref[:, :near_cols], back_img[:near_cols, cols],
                                    preferred_element_type=jnp.float32)
        near_wgt[:, cols] = jnp.dot(posts_ref[:, :near_cols], back_wgt[:near_cols, cols],
                                    preferred_element_type=jnp.float32)

    for t in range(2, n_img):
        place_posts(t)

    groups = img_rows // BLOCK
    group = lax.broadcasted_iota(jnp.int32, (1, img_rows), 1) // BLOCK
    placed = jnp.zeros((1, img_rows), jnp.float32)
    for t in range(n_img):
        plan = jnp.zeros((1, img_rows), jnp.int32)
        for g in range(groups):
            plan = jnp.where(group == g, plan_ref[img_from(t) * groups + g], plan)
        for s in range(groups):
            turned, target = evidence[t], plan
            if s:
                turned = pltpu.roll(evidence[t], s * BLOCK, 1)
                target = pltpu.roll(plan, s * BLOCK, 1)
            placed = placed + jnp.where(target == me * groups + group, turned, 0.0)
    ev_ref[...] = placed

    wait_bytes(every_stats.at[pl.ds(1, n_img * n_proj - 1)], stat_send)
    for n, every in enumerate((focus_all, limit_all)):
        wait_bytes(every.at[pl.ds(1, n_img - 1)], small_send.at[n])
    wait_bytes(every_terms.at[pl.ds(1, n_img - 1)], post_send)
    def far_bytes(rows):
        return moved.at[pl.ds(2, n_img - 2), pl.ds(0, rows)]

    wait_bytes(far_bytes(PIECES * PIECE + quarter + DIRECT), img_send)
    with jax.named_scope("quart"):
        wait_bytes(moved.at[pl.ds(2, n_img - 2), pl.ds(0, 3 * quarter)], pass_recv.at[0])
    for t in range(2, n_img):
        for rows in quarter_others:
            take_rows(t, rows)
    with jax.named_scope("half"):
        wait_bytes(far_bytes(PIECES * PIECE), pass_recv.at[1])
    for t in range(2, n_img):
        for rows in half_others:
            take_rows(t, rows)
    for t in range(2, n_img):
        with jax.named_scope(f"dir{t}"):
            move_img(t, PIECES + 1).wait_recv()
        take_rows(t, my_rows[PIECES + 1])
    wait_bytes(far_bytes(PIECES * PIECE + 3 * quarter), pass_send)


def back_kernel(near_cols, posts_ref, back_img, back_wgt, near_img, near_wgt, ev_ref, rec_hbm, placed_hbm, rec, out_sem):
    part = back_img.shape[1]
    steps = part // STEP
    posts = posts_ref[:, near_cols:]
    last = pltpu.make_async_copy(ev_ref, placed_hbm, out_sem.at[steps])
    last.start()
    copies = [last]
    for c in range(steps):
        cols = slice(c * STEP, (c + 1) * STEP)
        sums = near_img[:, cols] + jnp.dot(posts, back_img[near_cols:, cols], preferred_element_type=jnp.float32)
        weights = near_wgt[:, cols] + jnp.dot(posts, back_wgt[near_cols:, cols], preferred_element_type=jnp.float32)
        rec[:, cols] = (sums / (weights + 1.0)).astype(jnp.bfloat16)
        copies.append(pltpu.make_async_copy(rec.at[:, cols], rec_hbm.at[:, cols], out_sem.at[c]))
        copies[-1].start()
    for copy in copies:
        copy.wait()


def shards(n_img, n_proj, images, projections, noise_weight, defocus, orient_count, term_limit, block_plan):
    img_rows, width = images.shape
    proj_rows = projections.shape[0]
    part = width // n_img
    x_size = 1 << ((n_proj.bit_length() - 1) // 2)
    vmem = pl.BlockSpec(memory_space=pltpu.VMEM)
    hbm = pl.BlockSpec(memory_space=pl.ANY)
    bf16, f32, i32 = jnp.bfloat16, jnp.float32, jnp.int32
    dma, regular = pltpu.SemaphoreType.DMA, pltpu.SemaphoreType.REGULAR
    held = pl.pallas_call(
        functools.partial(score_kernel, n_img, n_proj, x_size),
        out_shape=(pltpu.VMEM((proj_rows, n_img * img_rows), bf16), pltpu.VMEM((n_img * img_rows, part), bf16),
                   pltpu.VMEM((n_img * img_rows, part), bf16), pltpu.VMEM((proj_rows, part), f32),
                   pltpu.VMEM((proj_rows, part), f32), pltpu.VMEM((1, img_rows), f32)),
        in_specs=[hbm] * 7,
        out_specs=(vmem,) * 6,
        scratch_shapes=[
            pltpu.VMEM((img_rows, width), bf16),
            pltpu.VMEM((proj_rows, width), bf16),
            pltpu.VMEM((1, width), f32),
            pltpu.VMEM((1, img_rows), f32),
            pltpu.VMEM((1, img_rows), i32),
            pltpu.VMEM((1, img_rows), i32),
            pltpu.SMEM(block_plan.shape, i32),
            pltpu.VMEM((2, img_rows, DEPTH), bf16),
            pltpu.VMEM((2, img_rows, DEPTH), bf16),
            pltpu.VMEM((proj_rows, img_rows), f32),
            pltpu.VMEM((4, img_rows, LANES), f32),
            pltpu.VMEM((n_img, img_rows, part), bf16),
            pltpu.VMEM((n_img * img_rows, part), f32),
            pltpu.VMEM((n_img, 1, img_rows), f32),
            pltpu.VMEM((n_img, 1, img_rows), i32),
            pltpu.VMEM((proj_rows, img_rows), bf16),
            pltpu.VMEM((n_img, proj_rows, img_rows), bf16),
            pltpu.VMEM((2, img_rows), f32),
            pltpu.VMEM((n_img * n_proj, 2, img_rows), f32),
            dma((5,)), dma((width // DEPTH // 2,)), dma((width // DEPTH // 2,)), regular, regular,
            dma((2,)), dma((2,)), dma((2,)), dma, dma((n_img - 2, PIECES + 2)), dma, dma((2,)),
            dma, dma((n_img - 1,)), dma, dma,
        ],
        compiler_params=pltpu.CompilerParams(
            collective_id=0, has_side_effects=True, vmem_limit_bytes=54 * 1024 * 1024),
    )(images, projections, noise_weight.reshape(1, -1), defocus.reshape(1, -1), orient_count.reshape(1, -1),
      term_limit.reshape(1, -1), block_plan)
    reconstruction, evidence = pl.pallas_call(
        functools.partial(back_kernel, 2 * img_rows),
        out_shape=(jax.ShapeDtypeStruct((proj_rows, part), bf16), jax.ShapeDtypeStruct((1, img_rows), f32)),
        in_specs=[vmem] * 6,
        out_specs=(hbm, hbm),
        scratch_shapes=[pltpu.VMEM((proj_rows, part), bf16), dma((part // STEP + 1,))],
        compiler_params=pltpu.CompilerParams(vmem_limit_bytes=16 * 1024 * 1024),
    )(*held)
    return reconstruction, evidence.reshape(-1)


def solution(mesh):
    n_img, n_proj = mesh.shape["img"], mesh.shape["proj"]
    placed = (P("img", None), P("proj", None), P(), P("img"), P("img"), P("img"), P())
    return jax.shard_map(
        functools.partial(shards, n_img, n_proj), mesh=mesh, in_specs=placed,
        out_specs=(P("proj", "img"), P("img")), check_vma=False,
    )
```

```python
import functools
import math

import jax
import jax.numpy as jnp
from jax import lax
from jax.experimental import pallas as pl
from jax.experimental.pallas import tpu as pltpu
from jax.sharding import PartitionSpec as P

BLOCK = 32
PIECES = 1
PIECE = 16
DIRECT = 32
STEP = 256
LANES = 128
DEPTH = 512
MESH = pl.DeviceIdType.MESH
SIN_TERMS = [(-1.0) ** k * math.pi ** (2 * k + 1) / math.factorial(2 * k + 1) for k in range(7)]
COS_TERMS = [(-1.0) ** k * math.pi ** (2 * k) / math.factorial(2 * k) for k in range(8)]


def horner(terms, x):
    total = jnp.full_like(x, terms[-1])
    for term in terms[-2::-1]:
        total = total * x + term
    return total


def sincos_turns(turns):
    rest = turns - jnp.floor(turns + 0.5)
    square = rest * rest
    half_sin = rest * horner(SIN_TERMS, square)
    half_cos = horner(COS_TERMS, square)
    return 2.0 * half_sin * half_cos, 1.0 - 2.0 * half_sin * half_sin


def columns_of(row, rows):
    return jnp.broadcast_to(row, (LANES, rows)).T


def step_sines(row, width):
    sin_d, cos_d = sincos_turns(row * (LANES / width))
    rows = row.shape[1]
    return columns_of(sin_d, rows), columns_of(cos_d, rows)


def sine_start(row, term0, width):
    sin_d, cos_d = step_sines(row, width)
    focus = columns_of(row, row.shape[1])
    sin0, cos0 = sincos_turns(focus * ((term0 + 1.0) / width) + 0.1 / (2.0 * math.pi))
    return sin0, sin0 * cos_d - cos0 * sin_d, 2.0 * cos_d


def wait_bytes(ref, sem):
    pltpu.make_async_copy(ref, ref, sem).wait()


def score_kernel(n_img, n_proj, x_size, img_hbm, proj_hbm, noise_hbm, focus_hbm, count_hbm, limit_hbm, plan_hbm,
                 posts_ref, back_img, back_wgt, near_img, near_wgt, ev_ref,
                 img, proj, noise_ref, focus_ref, count_ref, limit_ref, plan_ref, weighted, weighted_sq, total,
                 sine, moved, contrast, focus_all, limit_all, terms, every_terms, stats, every_stats,
                 load_sem, img_load, proj_load, next_token, all_token,
                 small_send, small_recv, near_sem, img_send, img_recv, pass_send, pass_recv,
                 post_send, post_recv, stat_send, stat_recv):
    me = lax.axis_index("img")
    mine = lax.axis_index("proj")
    img_rows, width = img.shape
    proj_rows = proj.shape[0]
    part = width // n_img
    chips = n_img // 2
    row_y, core = me // 2, lax.rem(me, 2)
    at_x, at_z = lax.rem(mine, x_size), mine // x_size

    def img_to(t):
        return lax.rem(row_y + t // 2, chips) * 2 + lax.rem(core + lax.rem(t, 2), 2)

    def img_from(t):
        return lax.rem(row_y + chips - t // 2, chips) * 2 + lax.rem(core + t % 2, 2)

    odd_x, odd_z = lax.rem(at_x, 2), lax.rem(at_z, 2)
    side = lax.rem(odd_x + odd_z, 2)
    beside_x, beside_z = mine + 1 - 2 * odd_x, mine + x_size * (1 - 2 * odd_z)
    beside_xz = beside_x + beside_z - mine
    quarter = (img_rows - 2 * PIECES * PIECE - DIRECT) // 4

    def half_rows(k, n):
        return pl.ds(pl.multiple_of((k * PIECES + n) * PIECE, PIECE), PIECE)

    def quarter_rows(x, z):
        return pl.ds(pl.multiple_of(2 * PIECES * PIECE + (x * 2 + z) * quarter, 8), quarter)

    def signal(sem, img, proj):
        pl.semaphore_signal(sem, inc=1, device_id={"img": img, "proj": proj}, device_id_type=MESH)

    barrier = pltpu.get_barrier_semaphore()
    partner, first_core = img_to(1), core == 0

    def greet_next(t, proj):
        signal(barrier, img_to(t) - lax.rem(img_to(t), 2), proj)

    for t in range(2, n_img, 2):
        greet_next(t, mine)
    pl.when(jnp.logical_not(first_core))(lambda: signal(barrier, partner, mine))

    def greet_all(proj, carry):
        for chip in range(chips):
            pl.when(jnp.logical_or(chip * 2 + 1 != me, proj != mine))(lambda: signal(barrier, chip * 2 + 1, proj))
        return carry

    def meet_all():
        with jax.named_scope("all"):
            @pl.when(jnp.logical_not(first_core))
            def _():
                pl.semaphore_wait(barrier, n_img * n_proj - 1)
                signal(all_token, partner, mine)
            pl.when(first_core)(lambda: pl.semaphore_wait(all_token, 1))

    small_loads = [pltpu.make_async_copy(source, target, load_sem.at[n]) for n, (source, target) in enumerate(
        ((focus_hbm, focus_ref), (limit_hbm, limit_ref), (noise_hbm, noise_ref), (count_hbm, count_ref),
         (plan_hbm, plan_ref)))]
    wide = 2 * DEPTH
    steps = width // wide

    def load_img(n):
        cols = pl.ds(pl.multiple_of(n * wide, wide), wide)
        return pltpu.make_async_copy(img_hbm.at[:, cols], img.at[:, cols], img_load.at[n])

    def load_proj(n):
        cols = pl.ds(pl.multiple_of(n * wide, wide), wide)
        return pltpu.make_async_copy(proj_hbm.at[:, cols], proj.at[:, cols], proj_load.at[n])

    for load in small_loads[:3]:
        load.start()
    load_img(0).start()
    for n in range(steps):
        load_proj(n).start()
        if n + 1 < steps:
            load_img(n + 1).start()
    for load in small_loads[3:]:
        load.start()
    with jax.named_scope('greet'):
        lax.fori_loop(0, n_proj, greet_all, 0)
    my_rows = [quarter_rows(odd_x, odd_z)] + [half_rows(side, n) for n in range(PIECES)]
    my_rows.append(pl.ds(img_rows - DIRECT, DIRECT))

    def move_img(t, n):
        slab = pl.ds(pl.multiple_of(img_to(t) * part, LANES), part)
        return pltpu.make_async_remote_copy(
            src_ref=img_hbm.at[my_rows[n], slab], dst_ref=moved.at[t, my_rows[n], :], send_sem=img_send,
            recv_sem=img_recv.at[t - 2, n], device_id={"img": img_to(t)}, device_id_type=MESH)

    def pass_rows(t, rows, proj, sem):
        held = moved.at[t, rows, :]
        pltpu.make_async_remote_copy(
            src_ref=held, dst_ref=held, send_sem=pass_send, recv_sem=sem, device_id={"proj": proj},
            device_id_type=MESH).start()

    near = pltpu.make_async_remote_copy(
        src_ref=img_hbm.at[:, pl.ds(pl.multiple_of(img_to(1) * part, LANES), part)], dst_ref=moved.at[1],
        send_sem=near_sem.at[0], recv_sem=near_sem.at[1], device_id={"img": img_to(1)}, device_id_type=MESH)
    small = [pltpu.make_async_remote_copy(
        src_ref=ref, dst_ref=dst.at[t], send_sem=small_send, recv_sem=small_recv,
        device_id={"img": img_to(t)}, device_id_type=MESH)
        for t in range(1, n_img) for ref, dst in ((focus_hbm, focus_all), (limit_hbm, limit_all))]
    far = [(t, n) for n in range(PIECES + 1) for t in range(2, n_img)]

    small_bytes = noise_ref.at[:, pl.ds(0, 2 * (n_img - 1) * img_rows)]

    def send_images():
        for copy in small:
            copy.start()
        for t, n in far:
            move_img(t, n).start()
        near.start()
        for t in range(2, n_img, 2):
            move_img(t, PIECES + 1).start()

    @pl.when(first_core)
    def _():
        with jax.named_scope("near"):
            pl.semaphore_wait(barrier, 2 * (chips - 1) + 1)
        signal(next_token, partner, mine)
        send_images()

    with jax.named_scope("small"):
        small_loads[0].wait()
        small_loads[1].wait()

    lane = lax.broadcasted_iota(jnp.int32, (1, LANES), 1).astype(jnp.float32)
    sine[0], sine[1], sine[2] = sine_start(focus_ref[...], lane, width)
    sine[3] = columns_of(limit_ref[...].astype(jnp.float32), img_rows)
    total[...] = jnp.zeros_like(total)
    small_loads[2].wait()
    contract = (((1,), (1,)), ((), ()))
    strip = 16

    def terms_chunk(c, slot):
        starts = [pl.multiple_of(c * DEPTH + k * LANES, LANES) for k in range(DEPTH // LANES)]
        noise = [noise_ref[:, pl.ds(start, LANES)] for start in starts]
        term = [lane + start.astype(jnp.float32) for start in starts]
        for r in range(img_rows // strip):
            rows = slice(r * strip, (r + 1) * strip)
            sin_v, sin_before, turn, limit = sine[0, rows], sine[1, rows], sine[2, rows], sine[3, rows]
            for k, start in enumerate(starts):
                cols = slice(k * LANES, (k + 1) * LANES)
                noisy = jnp.where(term[k] < limit, sin_v, 0.0) * noise[k]
                pixels = img[rows, pl.ds(start, LANES)].astype(jnp.float32)
                weighted[slot, rows, cols] = (noisy * pixels).astype(jnp.bfloat16)
                weighted_sq[slot, rows, cols] = (noisy * (-0.5 * sin_v)).astype(jnp.bfloat16)
                sin_v, sin_before = turn * sin_v - sin_before, sin_v
            sine[0, rows] = sin_v
            sine[1, rows] = sin_before

    def score_chunk(c, slot):
        rows = proj[:, pl.ds(pl.multiple_of(c * DEPTH, DEPTH), DEPTH)]
        got = lax.dot_general(rows, weighted[slot], contract, preferred_element_type=jnp.float32)
        return got + lax.dot_general(rows * rows, weighted_sq[slot], contract, preferred_element_type=jnp.float32)

    with jax.named_scope("img0"):
        load_img(0).wait()
    terms_chunk(jnp.int32(0), 0)

    def score_step(i, carry):
        with jax.named_scope("loads"):
            load_proj(i).wait()
            pl.when(i + 1 < steps)(lambda: load_img(i + 1).wait())

        @pl.when(jnp.logical_and(i == 0, jnp.logical_not(first_core)))
        def _():
            with jax.named_scope("near"):
                pl.semaphore_wait(next_token, 1)
            send_images()

        got = score_chunk(2 * i, 0)
        terms_chunk(2 * i + 1, 1)
        got = got + score_chunk(2 * i + 1, 1)
        terms_chunk(jnp.minimum(2 * i + 2, width // DEPTH - 1), 0)
        total[...] += got
        return carry

    lax.fori_loop(0, steps, score_step, 0)

    with jax.named_scope("smax"):
        small_loads[3].wait()
        small_loads[4].wait()
    scores = total[...]
    orient = lax.broadcasted_iota(jnp.int32, (proj_rows, img_rows), 0) + mine * proj_rows
    significant = orient < count_ref[...]
    masked = jnp.where(significant, scores, -1e30)
    peak = jnp.max(masked, axis=0, keepdims=True)
    expo = jnp.where(significant, jnp.exp(masked - peak), 0.0)
    stats[0:1, :] = peak
    stats[1:2, :] = jnp.sum(expo, axis=0, keepdims=True)
    terms[...] = expo.astype(jnp.bfloat16)

    rows_of = [img_to(t) for t in range(n_img)]

    def send_stats(target, carry):
        ahead = target - mine
        ahead = jnp.where(ahead < 0, ahead + n_proj, ahead)
        for t in range(n_img):
            copy = pltpu.make_async_remote_copy(
                src_ref=stats, dst_ref=every_stats.at[t * n_proj + ahead], send_sem=stat_send, recv_sem=stat_recv,
                device_id={"img": rows_of[t], "proj": target}, device_id_type=MESH)
            if t:
                copy.start()
            else:
                pl.when(target != mine)(copy.start)
        return carry

    def pass_on(t, n):
        with jax.named_scope(f"mv{t}{n}"):
            move_img(t, n).wait_recv()
        if n:
            pass_rows(t, my_rows[n], (beside_x, beside_z)[(n + t) % 2], pass_recv.at[1])
        else:
            for proj in (beside_xz, beside_x, beside_z):
                pass_rows(t, my_rows[0], proj, pass_recv.at[0])

    meet_all()
    with jax.named_scope("send"):
        lax.fori_loop(0, n_proj, send_stats, 0)

    post_copies = {t: pltpu.make_async_remote_copy(
        src_ref=terms, dst_ref=every_terms.at[t], send_sem=post_send, recv_sem=post_recv.at[t - 1],
        device_id={"img": img_to(t)}, device_id_type=MESH) for t in (1, *range(2, n_img, 2))}
    for t in range(2, n_img, 2):
        post_copies[t + 1] = pltpu.make_async_remote_copy(
            src_ref=every_terms.at[t], dst_ref=every_terms.at[t + 1], send_sem=post_send,
            recv_sem=post_recv.at[t], device_id={"img": img_to(1)}, device_id_type=MESH)
    post_copies[1].start()

    per_piece = n_img - 2
    for t, n in far[:per_piece]:
        pass_on(t, n)
    for t in range(2, n_img, 2):
        post_copies[t].start()
    for t in range(3, n_img, 2):
        move_img(t, PIECES + 1).start()

    term0 = lane + (me * part).astype(jnp.float32)

    def weights_block(t, carry):
        sine[0], sine[1], sine[2] = sine_start(focus_all[t], term0, width)
        sine[3] = columns_of(limit_all[t].astype(jnp.float32), img_rows)
        for r in range(img_rows // strip):
            inside = slice(r * strip, (r + 1) * strip)
            rows = pl.ds(pl.multiple_of(t * img_rows + r * strip, strip), strip)
            sin_v, sin_before, turn, limit = sine[0, inside], sine[1, inside], sine[2, inside], sine[3, inside]
            for c in range(part // LANES):
                cols = slice(c * LANES, (c + 1) * LANES)
                kept = jnp.where(term0 + float(c * LANES) < limit, sin_v, 0.0)
                contrast[rows, cols] = kept
                back_wgt[rows, cols] = (kept * sin_v).astype(jnp.bfloat16)
                sin_v, sin_before = turn * sin_v - sin_before, sin_v
        return carry

    def take_images(t, first, pixels):
        rows = pl.ds(pl.multiple_of(t * img_rows + first, 8), pixels.shape[0])
        back_img[rows, :] = (contrast[rows, :] * pixels.astype(jnp.float32)).astype(jnp.bfloat16)

    def take_rows(t, rows):
        take_images(t, rows.start, moved[t, rows, :])

    quarter_others = [quarter_rows(1 - odd_x, odd_z), quarter_rows(odd_x, 1 - odd_z), quarter_rows(1 - odd_x, 1 - odd_z)]
    half_others = [half_rows(1 - side, n) for n in range(PIECES)]

    focus_all[0] = focus_ref[...]
    limit_all[0] = limit_ref[...]
    fill_weights = lambda lo, hi: lax.fori_loop(lo, hi, weights_block, 0)
    fill_weights(0, 1)
    with jax.named_scope("smallx"):
        wait_bytes(small_bytes, small_recv)
    fill_weights(1, 2)
    fill_weights(2, 2 + per_piece // 2)
    for t, n in far[per_piece:2 * per_piece]:
        pass_on(t, n)
    fill_weights(2 + per_piece // 2, n_img)
    take_images(0, 0, img[:, pl.ds(pl.multiple_of(me * part, LANES), part)])
    with jax.named_scope("nearimg"):
        near.wait()
    take_images(1, 0, moved[1])
    for t, n in far[2 * per_piece:]:
        pass_on(t, n)
    for t in range(2, n_img, 2):
        with jax.named_scope(f"post{t}"):
            post_copies[t].wait_recv()
        post_copies[t + 1].start()
    for t, n in far:
        take_rows(t, my_rows[n])

    every_stats[0] = stats[...]
    with jax.named_scope("stat"):
        wait_bytes(every_stats.at[pl.ds(1, n_img * n_proj - 1)], stat_recv)
    evidence, scales = [], []
    for t in range(n_img):
        every = every_stats[pl.ds(t * n_proj, n_proj)]
        peaks, masses = every[:, 0, :], every[:, 1, :]
        highest = jnp.max(peaks, axis=0, keepdims=True)
        whole = jnp.sum(masses * jnp.exp(peaks - highest), axis=0, keepdims=True)
        evidence.append(highest + jnp.log(whole))
        scale = jnp.exp(peaks[0:1, :] - evidence[t])
        scales.append(scale)

    def place_posts(t):
        if t % 2:
            with jax.named_scope(f"post{t}"):
                post_copies[t].wait_recv()
        values = every_terms[t].astype(jnp.float32) if t else terms[...].astype(jnp.float32)
        posts_ref[:, t * img_rows:(t + 1) * img_rows] = (values * scales[t]).astype(jnp.bfloat16)

    for t in range(2):
        place_posts(t)
    near_cols = 2 * img_rows
    for c in range(part // STEP):
        cols = slice(c * STEP, (c + 1) * STEP)
        near_img[:, cols] = jnp.dot(posts_ref[:, :near_cols], back_img[:near_cols, cols],
                                    preferred_element_type=jnp.float32)
        near_wgt[:, cols] = jnp.dot(posts_ref[:, :near_cols], back_wgt[:near_cols, cols],
                                    preferred_element_type=jnp.float32)

    for t in range(2, n_img):
        place_posts(t)

    groups = img_rows // BLOCK
    group = lax.broadcasted_iota(jnp.int32, (1, img_rows), 1) // BLOCK
    placed = jnp.zeros((1, img_rows), jnp.float32)
    for t in range(n_img):
        plan = jnp.zeros((1, img_rows), jnp.int32)
        for g in range(groups):
            plan = jnp.where(group == g, plan_ref[img_from(t) * groups + g], plan)
        for s in range(groups):
            turned, target = evidence[t], plan
            if s:
                turned = pltpu.roll(evidence[t], s * BLOCK, 1)
                target = pltpu.roll(plan, s * BLOCK, 1)
            placed = placed + jnp.where(target == me * groups + group, turned, 0.0)
    ev_ref[...] = placed

    wait_bytes(every_stats.at[pl.ds(1, n_img * n_proj - 1)], stat_send)
    wait_bytes(small_bytes, small_send)
    wait_bytes(every_terms.at[pl.ds(1, n_img - 1)], post_send)
    def far_bytes(rows):
        return moved.at[pl.ds(2, n_img - 2), pl.ds(0, rows)]

    wait_bytes(far_bytes(PIECES * PIECE + quarter + DIRECT), img_send)
    with jax.named_scope("quart"):
        wait_bytes(moved.at[pl.ds(2, n_img - 2), pl.ds(0, 3 * quarter)], pass_recv.at[0])
    for t in range(2, n_img):
        for rows in quarter_others:
            take_rows(t, rows)
    with jax.named_scope("half"):
        wait_bytes(far_bytes(PIECES * PIECE), pass_recv.at[1])
    for t in range(2, n_img):
        for rows in half_others:
            take_rows(t, rows)
    for t in range(2, n_img):
        with jax.named_scope(f"dir{t}"):
            move_img(t, PIECES + 1).wait_recv()
        take_rows(t, my_rows[PIECES + 1])
    wait_bytes(far_bytes(PIECES * PIECE + 3 * quarter), pass_send)


def back_kernel(near_cols, posts_ref, back_img, back_wgt, near_img, near_wgt, ev_ref, rec_hbm, placed_hbm, rec, out_sem):
    part = back_img.shape[1]
    steps = part // STEP
    posts = posts_ref[:, near_cols:]
    last = pltpu.make_async_copy(ev_ref, placed_hbm, out_sem.at[1])
    last.start()
    for c in range(steps):
        cols = slice(c * STEP, (c + 1) * STEP)
        sums = near_img[:, cols] + jnp.dot(posts, back_img[near_cols:, cols], preferred_element_type=jnp.float32)
        weights = near_wgt[:, cols] + jnp.dot(posts, back_wgt[near_cols:, cols], preferred_element_type=jnp.float32)
        rec[:, cols] = (sums / (weights + 1.0)).astype(jnp.bfloat16)
        pltpu.make_async_copy(rec.at[:, cols], rec_hbm.at[:, cols], out_sem.at[0]).start()
    pltpu.make_async_copy(rec, rec_hbm, out_sem.at[0]).wait()
    last.wait()


def shards(n_img, n_proj, images, projections, noise_weight, defocus, orient_count, term_limit, block_plan):
    img_rows, width = images.shape
    proj_rows = projections.shape[0]
    part = width // n_img
    x_size = 1 << ((n_proj.bit_length() - 1) // 2)
    vmem = pl.BlockSpec(memory_space=pltpu.VMEM)
    hbm = pl.BlockSpec(memory_space=pl.ANY)
    bf16, f32, i32 = jnp.bfloat16, jnp.float32, jnp.int32
    dma, regular = pltpu.SemaphoreType.DMA, pltpu.SemaphoreType.REGULAR
    held = pl.pallas_call(
        functools.partial(score_kernel, n_img, n_proj, x_size),
        out_shape=(pltpu.VMEM((proj_rows, n_img * img_rows), bf16), pltpu.VMEM((n_img * img_rows, part), bf16),
                   pltpu.VMEM((n_img * img_rows, part), bf16), pltpu.VMEM((proj_rows, part), f32),
                   pltpu.VMEM((proj_rows, part), f32), pltpu.VMEM((1, img_rows), f32)),
        in_specs=[hbm] * 7,
        out_specs=(vmem,) * 6,
        scratch_shapes=[
            pltpu.VMEM((img_rows, width), bf16),
            pltpu.VMEM((proj_rows, width), bf16),
            pltpu.VMEM((1, width), f32),
            pltpu.VMEM((1, img_rows), f32),
            pltpu.VMEM((1, img_rows), i32),
            pltpu.VMEM((1, img_rows), i32),
            pltpu.SMEM(block_plan.shape, i32),
            pltpu.VMEM((2, img_rows, DEPTH), bf16),
            pltpu.VMEM((2, img_rows, DEPTH), bf16),
            pltpu.VMEM((proj_rows, img_rows), f32),
            pltpu.VMEM((4, img_rows, LANES), f32),
            pltpu.VMEM((n_img, img_rows, part), bf16),
            pltpu.VMEM((n_img * img_rows, part), f32),
            pltpu.VMEM((n_img, 1, img_rows), f32),
            pltpu.VMEM((n_img, 1, img_rows), i32),
            pltpu.VMEM((proj_rows, img_rows), bf16),
            pltpu.VMEM((n_img, proj_rows, img_rows), bf16),
            pltpu.VMEM((2, img_rows), f32),
            pltpu.VMEM((n_img * n_proj, 2, img_rows), f32),
            dma((5,)), dma((width // DEPTH // 2,)), dma((width // DEPTH // 2,)), regular, regular,
            dma, dma, dma((2,)), dma, dma((n_img - 2, PIECES + 2)), dma, dma((2,)),
            dma, dma((n_img - 1,)), dma, dma,
        ],
        compiler_params=pltpu.CompilerParams(
            collective_id=0, has_side_effects=True, vmem_limit_bytes=54 * 1024 * 1024),
    )(images, projections, noise_weight.reshape(1, -1), defocus.reshape(1, -1), orient_count.reshape(1, -1),
      term_limit.reshape(1, -1), block_plan)
    reconstruction, evidence = pl.pallas_call(
        functools.partial(back_kernel, 2 * img_rows),
        out_shape=(jax.ShapeDtypeStruct((proj_rows, part), bf16), jax.ShapeDtypeStruct((1, img_rows), f32)),
        in_specs=[vmem] * 6,
        out_specs=(hbm, hbm),
        scratch_shapes=[pltpu.VMEM((proj_rows, part), bf16), dma((2,))],
        compiler_params=pltpu.CompilerParams(vmem_limit_bytes=16 * 1024 * 1024),
    )(*held)
    return reconstruction, evidence.reshape(-1)


def solution(mesh):
    n_img, n_proj = mesh.shape["img"], mesh.shape["proj"]
    placed = (P("img", None), P("proj", None), P(), P("img"), P("img"), P("img"), P())
    return jax.shard_map(
        functools.partial(shards, n_img, n_proj), mesh=mesh, in_specs=placed,
        out_specs=(P("proj", "img"), P("img")), check_vma=False,
    )
```

```python
import functools
import math

import jax
import jax.numpy as jnp
from jax import lax
from jax.experimental import pallas as pl
from jax.experimental.pallas import tpu as pltpu
from jax.sharding import PartitionSpec as P

BLOCK = 32
PIECES = 1
PIECE = 16
DIRECT = 32
STEP = 256
LANES = 128
DEPTH = 512
MESH = pl.DeviceIdType.MESH
SIN_TERMS = [(-1.0) ** k * math.pi ** (2 * k + 1) / math.factorial(2 * k + 1) for k in range(7)]
COS_TERMS = [(-1.0) ** k * math.pi ** (2 * k) / math.factorial(2 * k) for k in range(8)]


def horner(terms, x):
    total = jnp.full_like(x, terms[-1])
    for term in terms[-2::-1]:
        total = total * x + term
    return total


def sincos_turns(turns):
    rest = turns - jnp.floor(turns + 0.5)
    square = rest * rest
    half_sin = rest * horner(SIN_TERMS, square)
    half_cos = horner(COS_TERMS, square)
    return 2.0 * half_sin * half_cos, 1.0 - 2.0 * half_sin * half_sin


def columns_of(row, rows):
    return jnp.broadcast_to(row, (LANES, rows)).T


def step_sines(row, width):
    sin_d, cos_d = sincos_turns(row * (LANES / width))
    rows = row.shape[1]
    return columns_of(sin_d, rows), columns_of(cos_d, rows)


def sine_start(row, term0, width):
    sin_d, cos_d = step_sines(row, width)
    focus = columns_of(row, row.shape[1])
    sin0, cos0 = sincos_turns(focus * ((term0 + 1.0) / width) + 0.1 / (2.0 * math.pi))
    return sin0, sin0 * cos_d - cos0 * sin_d, 2.0 * cos_d


def wait_bytes(ref, sem):
    pltpu.make_async_copy(ref, ref, sem).wait()


def score_kernel(n_img, n_proj, x_size, img_hbm, proj_hbm, noise_hbm, focus_hbm, count_hbm, limit_hbm, plan_hbm,
                 posts_ref, back_img, back_wgt, near_img, near_wgt, ev_ref,
                 img, proj, noise_ref, focus_ref, count_ref, limit_ref, plan_ref, weighted, weighted_sq, total,
                 sine, moved, contrast, focus_all, limit_all, terms, every_terms, stats, every_stats,
                 load_sem, img_load, proj_load, next_token, all_token,
                 small_send, small_recv, near_sem, img_send, img_recv, pass_send, pass_recv,
                 post_send, post_recv, stat_send, stat_recv):
    me = lax.axis_index("img")
    mine = lax.axis_index("proj")
    img_rows, width = img.shape
    proj_rows = proj.shape[0]
    part = width // n_img
    chips = n_img // 2
    row_y, core = me // 2, lax.rem(me, 2)
    at_x, at_z = lax.rem(mine, x_size), mine // x_size

    def img_to(t):
        return lax.rem(row_y + t // 2, chips) * 2 + lax.rem(core + lax.rem(t, 2), 2)

    def img_from(t):
        return lax.rem(row_y + chips - t // 2, chips) * 2 + lax.rem(core + t % 2, 2)

    odd_x, odd_z = lax.rem(at_x, 2), lax.rem(at_z, 2)
    side = lax.rem(odd_x + odd_z, 2)
    beside_x, beside_z = mine + 1 - 2 * odd_x, mine + x_size * (1 - 2 * odd_z)
    beside_xz = beside_x + beside_z - mine
    quarter = (img_rows - 2 * PIECES * PIECE - DIRECT) // 4

    def half_rows(k, n):
        return pl.ds(pl.multiple_of((k * PIECES + n) * PIECE, PIECE), PIECE)

    def quarter_rows(x, z):
        return pl.ds(pl.multiple_of(2 * PIECES * PIECE + (x * 2 + z) * quarter, 8), quarter)

    def signal(sem, img, proj):
        pl.semaphore_signal(sem, inc=1, device_id={"img": img, "proj": proj}, device_id_type=MESH)

    barrier = pltpu.get_barrier_semaphore()
    partner, first_core = img_to(1), core == 0

    def greet_next(t, proj):
        signal(barrier, img_to(t) - lax.rem(img_to(t), 2), proj)

    for t in range(2, n_img, 2):
        greet_next(t, mine)
    pl.when(jnp.logical_not(first_core))(lambda: signal(barrier, partner, mine))

    def greet_all(proj, carry):
        for chip in range(chips):
            pl.when(jnp.logical_or(chip * 2 + 1 != me, proj != mine))(lambda: signal(barrier, chip * 2 + 1, proj))
        return carry

    def meet_all():
        with jax.named_scope("all"):
            @pl.when(jnp.logical_not(first_core))
            def _():
                pl.semaphore_wait(barrier, n_img * n_proj - 1)
                signal(all_token, partner, mine)
            pl.when(first_core)(lambda: pl.semaphore_wait(all_token, 1))

    small_loads = [pltpu.make_async_copy(source, target, load_sem.at[n]) for n, source, target in (
        (0, focus_hbm, focus_ref), (0, limit_hbm, limit_ref), (1, noise_hbm, noise_ref), (2, count_hbm, count_ref),
        (3, plan_hbm, plan_ref))]
    wide = 2 * DEPTH
    steps = width // wide

    def load_img(n):
        cols = pl.ds(pl.multiple_of(n * wide, wide), wide)
        return pltpu.make_async_copy(img_hbm.at[:, cols], img.at[:, cols], img_load.at[n])

    def load_proj(n):
        cols = pl.ds(pl.multiple_of(n * wide, wide), wide)
        return pltpu.make_async_copy(proj_hbm.at[:, cols], proj.at[:, cols], proj_load.at[n])

    for load in small_loads[:3]:
        load.start()
    load_img(0).start()
    for n in range(steps):
        load_proj(n).start()
        if n + 1 < steps:
            load_img(n + 1).start()
    for load in small_loads[3:]:
        load.start()
    with jax.named_scope('greet'):
        lax.fori_loop(0, n_proj, greet_all, 0)
    my_rows = [quarter_rows(odd_x, odd_z)] + [half_rows(side, n) for n in range(PIECES)]
    my_rows.append(pl.ds(img_rows - DIRECT, DIRECT))

    def move_img(t, n):
        slab = pl.ds(pl.multiple_of(img_to(t) * part, LANES), part)
        return pltpu.make_async_remote_copy(
            src_ref=img_hbm.at[my_rows[n], slab], dst_ref=moved.at[t, my_rows[n], :], send_sem=img_send,
            recv_sem=img_recv.at[t - 2, n], device_id={"img": img_to(t)}, device_id_type=MESH)

    def pass_rows(t, rows, proj, sem):
        held = moved.at[t, rows, :]
        pltpu.make_async_remote_copy(
            src_ref=held, dst_ref=held, send_sem=pass_send, recv_sem=sem, device_id={"proj": proj},
            device_id_type=MESH).start()

    near = pltpu.make_async_remote_copy(
        src_ref=img_hbm.at[:, pl.ds(pl.multiple_of(img_to(1) * part, LANES), part)], dst_ref=moved.at[1],
        send_sem=near_sem.at[0], recv_sem=near_sem.at[1], device_id={"img": img_to(1)}, device_id_type=MESH)
    small = [pltpu.make_async_remote_copy(
        src_ref=ref, dst_ref=dst.at[t], send_sem=small_send, recv_sem=small_recv,
        device_id={"img": img_to(t)}, device_id_type=MESH)
        for t in range(1, n_img) for ref, dst in ((focus_hbm, focus_all), (limit_hbm, limit_all))]
    far = [(t, n) for n in range(PIECES + 1) for t in range(2, n_img)]

    small_bytes = noise_ref.at[:, pl.ds(0, 2 * (n_img - 1) * img_rows)]

    def send_images():
        for copy in small:
            copy.start()
        for t, n in far:
            move_img(t, n).start()
        near.start()
        for t in range(2, n_img, 2):
            move_img(t, PIECES + 1).start()

    @pl.when(first_core)
    def _():
        with jax.named_scope("near"):
            pl.semaphore_wait(barrier, 2 * (chips - 1) + 1)
        signal(next_token, partner, mine)
        send_images()

    with jax.named_scope("small"):
        wait_bytes(focus_all.at[pl.ds(0, 2)], load_sem.at[0])

    lane = lax.broadcasted_iota(jnp.int32, (1, LANES), 1).astype(jnp.float32)
    sine[0], sine[1], sine[2] = sine_start(focus_ref[...], lane, width)
    sine[3] = columns_of(limit_ref[...].astype(jnp.float32), img_rows)
    total[...] = jnp.zeros_like(total)
    small_loads[2].wait()
    contract = (((1,), (1,)), ((), ()))
    strip = 16

    def terms_chunk(c, slot):
        starts = [pl.multiple_of(c * DEPTH + k * LANES, LANES) for k in range(DEPTH // LANES)]
        noise = [noise_ref[:, pl.ds(start, LANES)] for start in starts]
        term = [lane + start.astype(jnp.float32) for start in starts]
        for r in range(img_rows // strip):
            rows = slice(r * strip, (r + 1) * strip)
            sin_v, sin_before, turn, limit = sine[0, rows], sine[1, rows], sine[2, rows], sine[3, rows]
            for k, start in enumerate(starts):
                cols = slice(k * LANES, (k + 1) * LANES)
                noisy = jnp.where(term[k] < limit, sin_v, 0.0) * noise[k]
                pixels = img[rows, pl.ds(start, LANES)].astype(jnp.float32)
                weighted[slot, rows, cols] = (noisy * pixels).astype(jnp.bfloat16)
                weighted_sq[slot, rows, cols] = (noisy * (-0.5 * sin_v)).astype(jnp.bfloat16)
                sin_v, sin_before = turn * sin_v - sin_before, sin_v
            sine[0, rows] = sin_v
            sine[1, rows] = sin_before

    def score_chunk(c, slot):
        rows = proj[:, pl.ds(pl.multiple_of(c * DEPTH, DEPTH), DEPTH)]
        got = lax.dot_general(rows, weighted[slot], contract, preferred_element_type=jnp.float32)
        return got + lax.dot_general(rows * rows, weighted_sq[slot], contract, preferred_element_type=jnp.float32)

    with jax.named_scope("img0"):
        load_img(0).wait()
    terms_chunk(jnp.int32(0), 0)

    def score_step(i, carry):
        with jax.named_scope("loads"):
            load_proj(i).wait()
            pl.when(i + 1 < steps)(lambda: load_img(i + 1).wait())

        @pl.when(jnp.logical_and(i == 0, jnp.logical_not(first_core)))
        def _():
            with jax.named_scope("near"):
                pl.semaphore_wait(next_token, 1)
            send_images()

        got = score_chunk(2 * i, 0)
        terms_chunk(2 * i + 1, 1)
        got = got + score_chunk(2 * i + 1, 1)
        terms_chunk(jnp.minimum(2 * i + 2, width // DEPTH - 1), 0)
        total[...] += got
        return carry

    lax.fori_loop(0, steps, score_step, 0)

    with jax.named_scope("smax"):
        small_loads[3].wait()
        small_loads[4].wait()
    scores = total[...]
    orient = lax.broadcasted_iota(jnp.int32, (proj_rows, img_rows), 0) + mine * proj_rows
    significant = orient < count_ref[...]
    masked = jnp.where(significant, scores, -1e30)
    peak = jnp.max(masked, axis=0, keepdims=True)
    expo = jnp.where(significant, jnp.exp(masked - peak), 0.0)
    stats[0:1, :] = peak
    stats[1:2, :] = jnp.sum(expo, axis=0, keepdims=True)
    terms[...] = expo.astype(jnp.bfloat16)

    rows_of = [img_to(t) for t in range(n_img)]

    def send_stats(target, carry):
        ahead = target - mine
        ahead = jnp.where(ahead < 0, ahead + n_proj, ahead)
        for t in range(n_img):
            copy = pltpu.make_async_remote_copy(
                src_ref=stats, dst_ref=every_stats.at[t * n_proj + ahead], send_sem=stat_send, recv_sem=stat_recv,
                device_id={"img": rows_of[t], "proj": target}, device_id_type=MESH)
            if t:
                copy.start()
            else:
                pl.when(target != mine)(copy.start)
        return carry

    def pass_on(t, n):
        with jax.named_scope(f"mv{t}{n}"):
            move_img(t, n).wait_recv()
        if n:
            pass_rows(t, my_rows[n], (beside_x, beside_z)[(n + t) % 2], pass_recv.at[1])
        else:
            for proj in (beside_xz, beside_x, beside_z):
                pass_rows(t, my_rows[0], proj, pass_recv.at[0])

    meet_all()
    with jax.named_scope("send"):
        lax.fori_loop(0, n_proj, send_stats, 0)

    post_copies = {t: pltpu.make_async_remote_copy(
        src_ref=terms, dst_ref=every_terms.at[t], send_sem=post_send, recv_sem=post_recv.at[t - 1],
        device_id={"img": img_to(t)}, device_id_type=MESH) for t in (1, *range(2, n_img, 2))}
    for t in range(2, n_img, 2):
        post_copies[t + 1] = pltpu.make_async_remote_copy(
            src_ref=every_terms.at[t], dst_ref=every_terms.at[t + 1], send_sem=post_send,
            recv_sem=post_recv.at[t], device_id={"img": img_to(1)}, device_id_type=MESH)
    post_copies[1].start()

    per_piece = n_img - 2
    for t in range(2, n_img, 2):
        post_copies[t].start()
    for t, n in far[:per_piece]:
        pass_on(t, n)
    for t in range(3, n_img, 2):
        move_img(t, PIECES + 1).start()

    term0 = lane + (me * part).astype(jnp.float32)

    def weights_block(t, carry):
        sine[0], sine[1], sine[2] = sine_start(focus_all[t], term0, width)
        sine[3] = columns_of(limit_all[t].astype(jnp.float32), img_rows)
        for r in range(img_rows // strip):
            inside = slice(r * strip, (r + 1) * strip)
            rows = pl.ds(pl.multiple_of(t * img_rows + r * strip, strip), strip)
            sin_v, sin_before, turn, limit = sine[0, inside], sine[1, inside], sine[2, inside], sine[3, inside]
            for c in range(part // LANES):
                cols = slice(c * LANES, (c + 1) * LANES)
                kept = jnp.where(term0 + float(c * LANES) < limit, sin_v, 0.0)
                contrast[rows, cols] = kept
                back_wgt[rows, cols] = (kept * sin_v).astype(jnp.bfloat16)
                sin_v, sin_before = turn * sin_v - sin_before, sin_v
        return carry

    def take_images(t, first, pixels):
        rows = pl.ds(pl.multiple_of(t * img_rows + first, 8), pixels.shape[0])
        back_img[rows, :] = (contrast[rows, :] * pixels.astype(jnp.float32)).astype(jnp.bfloat16)

    def take_rows(t, rows):
        take_images(t, rows.start, moved[t, rows, :])

    quarter_others = [quarter_rows(1 - odd_x, odd_z), quarter_rows(odd_x, 1 - odd_z), quarter_rows(1 - odd_x, 1 - odd_z)]
    half_others = [half_rows(1 - side, n) for n in range(PIECES)]

    focus_all[0] = focus_ref[...]
    limit_all[0] = limit_ref[...]
    fill_weights = lambda lo, hi: lax.fori_loop(lo, hi, weights_block, 0)
    fill_weights(0, 1)
    with jax.named_scope("smallx"):
        wait_bytes(small_bytes, small_recv)
    fill_weights(1, 2)
    fill_weights(2, 2 + per_piece // 2)
    for t, n in far[per_piece:2 * per_piece]:
        pass_on(t, n)
    fill_weights(2 + per_piece // 2, n_img)
    take_images(0, 0, img[:, pl.ds(pl.multiple_of(me * part, LANES), part)])
    with jax.named_scope("nearimg"):
        near.wait()
    take_images(1, 0, moved[1])
    for t, n in far[2 * per_piece:]:
        pass_on(t, n)
    for t in range(2, n_img, 2):
        with jax.named_scope(f"post{t}"):
            post_copies[t].wait_recv()
        post_copies[t + 1].start()
    for t, n in far:
        take_rows(t, my_rows[n])

    every_stats[0] = stats[...]
    with jax.named_scope("stat"):
        wait_bytes(every_stats.at[pl.ds(1, n_img * n_proj - 1)], stat_recv)
    evidence, scales = [], []
    for t in range(n_img):
        every = every_stats[pl.ds(t * n_proj, n_proj)]
        peaks, masses = every[:, 0, :], every[:, 1, :]
        highest = jnp.max(peaks, axis=0, keepdims=True)
        whole = jnp.sum(masses * jnp.exp(peaks - highest), axis=0, keepdims=True)
        evidence.append(highest + jnp.log(whole))
        scale = jnp.exp(peaks[0:1, :] - evidence[t])
        scales.append(scale)

    def place_posts(t):
        if t % 2:
            with jax.named_scope(f"post{t}"):
                post_copies[t].wait_recv()
        values = every_terms[t].astype(jnp.float32) if t else terms[...].astype(jnp.float32)
        posts_ref[:, t * img_rows:(t + 1) * img_rows] = (values * scales[t]).astype(jnp.bfloat16)

    for t in range(2):
        place_posts(t)
    near_cols = 2 * img_rows
    for c in range(part // STEP):
        cols = slice(c * STEP, (c + 1) * STEP)
        near_img[:, cols] = jnp.dot(posts_ref[:, :near_cols], back_img[:near_cols, cols],
                                    preferred_element_type=jnp.float32)
        near_wgt[:, cols] = jnp.dot(posts_ref[:, :near_cols], back_wgt[:near_cols, cols],
                                    preferred_element_type=jnp.float32)

    for t in range(2, n_img):
        place_posts(t)

    groups = img_rows // BLOCK
    group = lax.broadcasted_iota(jnp.int32, (1, img_rows), 1) // BLOCK
    placed = jnp.zeros((1, img_rows), jnp.float32)
    for t in range(n_img):
        plan = jnp.zeros((1, img_rows), jnp.int32)
        for g in range(groups):
            plan = jnp.where(group == g, plan_ref[img_from(t) * groups + g], plan)
        for s in range(groups):
            turned, target = evidence[t], plan
            if s:
                turned = pltpu.roll(evidence[t], s * BLOCK, 1)
                target = pltpu.roll(plan, s * BLOCK, 1)
            placed = placed + jnp.where(target == me * groups + group, turned, 0.0)
    ev_ref[...] = placed

    wait_bytes(every_stats.at[pl.ds(1, n_img * n_proj - 1)], stat_send)
    wait_bytes(small_bytes, small_send)
    wait_bytes(every_terms.at[pl.ds(1, n_img - 1)], post_send)
    def far_bytes(rows):
        return moved.at[pl.ds(2, n_img - 2), pl.ds(0, rows)]

    wait_bytes(far_bytes(PIECES * PIECE + quarter + DIRECT), img_send)
    with jax.named_scope("quart"):
        wait_bytes(moved.at[pl.ds(2, n_img - 2), pl.ds(0, 3 * quarter)], pass_recv.at[0])
    for t in range(2, n_img):
        for rows in quarter_others:
            take_rows(t, rows)
    with jax.named_scope("half"):
        wait_bytes(far_bytes(PIECES * PIECE), pass_recv.at[1])
    for t in range(2, n_img):
        for rows in half_others:
            take_rows(t, rows)
    for t in range(2, n_img):
        with jax.named_scope(f"dir{t}"):
            move_img(t, PIECES + 1).wait_recv()
        take_rows(t, my_rows[PIECES + 1])
    wait_bytes(far_bytes(PIECES * PIECE + 3 * quarter), pass_send)


def back_kernel(near_cols, posts_ref, back_img, back_wgt, near_img, near_wgt, ev_ref, rec_hbm, placed_hbm, rec, out_sem):
    part = back_img.shape[1]
    steps = part // STEP
    posts = posts_ref[:, near_cols:]
    last = pltpu.make_async_copy(ev_ref, placed_hbm, out_sem.at[1])
    last.start()
    for c in range(steps):
        cols = slice(c * STEP, (c + 1) * STEP)
        sums = near_img[:, cols] + jnp.dot(posts, back_img[near_cols:, cols], preferred_element_type=jnp.float32)
        weights = near_wgt[:, cols] + jnp.dot(posts, back_wgt[near_cols:, cols], preferred_element_type=jnp.float32)
        rec[:, cols] = (sums / (weights + 1.0)).astype(jnp.bfloat16)
        pltpu.make_async_copy(rec.at[:, cols], rec_hbm.at[:, cols], out_sem.at[0]).start()
    pltpu.make_async_copy(rec, rec_hbm, out_sem.at[0]).wait()
    last.wait()


def shards(n_img, n_proj, images, projections, noise_weight, defocus, orient_count, term_limit, block_plan):
    img_rows, width = images.shape
    proj_rows = projections.shape[0]
    part = width // n_img
    x_size = 1 << ((n_proj.bit_length() - 1) // 2)
    vmem = pl.BlockSpec(memory_space=pltpu.VMEM)
    hbm = pl.BlockSpec(memory_space=pl.ANY)
    bf16, f32, i32 = jnp.bfloat16, jnp.float32, jnp.int32
    dma, regular = pltpu.SemaphoreType.DMA, pltpu.SemaphoreType.REGULAR
    held = pl.pallas_call(
        functools.partial(score_kernel, n_img, n_proj, x_size),
        out_shape=(pltpu.VMEM((proj_rows, n_img * img_rows), bf16), pltpu.VMEM((n_img * img_rows, part), bf16),
                   pltpu.VMEM((n_img * img_rows, part), bf16), pltpu.VMEM((proj_rows, part), f32),
                   pltpu.VMEM((proj_rows, part), f32), pltpu.VMEM((1, img_rows), f32)),
        in_specs=[hbm] * 7,
        out_specs=(vmem,) * 6,
        scratch_shapes=[
            pltpu.VMEM((img_rows, width), bf16),
            pltpu.VMEM((proj_rows, width), bf16),
            pltpu.VMEM((1, width), f32),
            pltpu.VMEM((1, img_rows), f32),
            pltpu.VMEM((1, img_rows), i32),
            pltpu.VMEM((1, img_rows), i32),
            pltpu.SMEM(block_plan.shape, i32),
            pltpu.VMEM((2, img_rows, DEPTH), bf16),
            pltpu.VMEM((2, img_rows, DEPTH), bf16),
            pltpu.VMEM((proj_rows, img_rows), f32),
            pltpu.VMEM((4, img_rows, LANES), f32),
            pltpu.VMEM((n_img, img_rows, part), bf16),
            pltpu.VMEM((n_img * img_rows, part), f32),
            pltpu.VMEM((n_img, 1, img_rows), f32),
            pltpu.VMEM((n_img, 1, img_rows), i32),
            pltpu.VMEM((proj_rows, img_rows), bf16),
            pltpu.VMEM((n_img, proj_rows, img_rows), bf16),
            pltpu.VMEM((2, img_rows), f32),
            pltpu.VMEM((n_img * n_proj, 2, img_rows), f32),
            dma((4,)), dma((width // DEPTH // 2,)), dma((width // DEPTH // 2,)), regular, regular,
            dma, dma, dma((2,)), dma, dma((n_img - 2, PIECES + 2)), dma, dma((2,)),
            dma, dma((n_img - 1,)), dma, dma,
        ],
        compiler_params=pltpu.CompilerParams(
            collective_id=0, has_side_effects=True, vmem_limit_bytes=54 * 1024 * 1024),
    )(images, projections, noise_weight.reshape(1, -1), defocus.reshape(1, -1), orient_count.reshape(1, -1),
      term_limit.reshape(1, -1), block_plan)
    reconstruction, evidence = pl.pallas_call(
        functools.partial(back_kernel, 2 * img_rows),
        out_shape=(jax.ShapeDtypeStruct((proj_rows, part), bf16), jax.ShapeDtypeStruct((1, img_rows), f32)),
        in_specs=[vmem] * 6,
        out_specs=(hbm, hbm),
        scratch_shapes=[pltpu.VMEM((proj_rows, part), bf16), dma((2,))],
        compiler_params=pltpu.CompilerParams(vmem_limit_bytes=16 * 1024 * 1024),
    )(*held)
    return reconstruction, evidence.reshape(-1)


def solution(mesh):
    n_img, n_proj = mesh.shape["img"], mesh.shape["proj"]
    placed = (P("img", None), P("proj", None), P(), P("img"), P("img"), P("img"), P())
    return jax.shard_map(
        functools.partial(shards, n_img, n_proj), mesh=mesh, in_specs=placed,
        out_specs=(P("proj", "img"), P("img")), check_vma=False,
    )
```
